32 devices in a mesh: member: 2 (over x), lat: 16 (over z, y, core).
Axes of the slice: x: 2, y: 2, z: 4, core: 2. Of those that a mesh axis runs over, the one named last changes fastest.
Arguments:
- field: bfloat16 [192, 1440, 256], P(('member', 'lat')), parts along dimension 0, may hold values from -3000 to 3000
- gain: float32 [256], replicated, may hold values from 0.1 to 1.9
- slot_wave: int32 [96], replicated, may hold values from 0 to 96, as said below
- legendre: bfloat16 [96, 96, 96], P('lat'), may hold values from -0.625 to 0.625
- mixing: bfloat16 [96, 2, 256, 256], P('lat'), may hold values from -0.25 to 0.25
Outputs:
- result: bfloat16 [192, 1440, 256], P(('member', 'lat')), parts along dimension 0
The draws below stay inside these ranges and needn't reach their ends.
There are 2 independent parts, one for each index of `member`. The reference program is written for one: setup_inputs(seed, part) draws one part's arguments, and reference() takes and returns one part's arrays. A program takes and returns all parts, laid end to end along the dimension named above; an argument that names none is the same for every part. Nothing has to cross between parts.
Inputs may be any that keep to these rules, and one draw needn't show every extreme that they name: `slot_wave`: each wavenumber 0 to 95 stands in exactly one slot and every other slot holds 96; slots 2k and 2k+1 of one lat index hold wavenumbers adding up to (4k+2)16 - 1 where both are below 96.
All inputs are finite; a program needn't handle non-finite values.
Results may differ from the reference program's by a relative error of at most 0.0085.
Values may be sent and summed in bfloat16 or wider, within the bound.
A program may use at most 64 MiB of HBM per device.

```python
import math
import jax
import jax.numpy as jnp
from jax import lax

C = 256
NLON = 1440
NLAT = 96
DEG = 96
SLOT_DEV = 6
SLOTS = 96
N_LAT = 16


def draw_field(key, part):
    keys = jax.random.split(key, 3)
    rows = jnp.arange(NLAT, dtype=jnp.float32) / NLAT
    wobble = 0.3 * jax.random.normal(keys[0], (NLAT,), jnp.float32)
    chan = 10.0 ** jax.random.uniform(keys[1], (C,), jnp.float32, 0.0, 1.0)
    base = jnp.clip(jax.random.normal(keys[2], (NLAT, NLON, C), jnp.float32), -6.0, 6.0)
    row_exp = rows + wobble
    row_exp = jnp.clip(row_exp, -0.5, 1.5)
    values = base * (10.0 ** row_exp)[:, None, None] * chan[None, None, :]
    return values.astype(jnp.bfloat16)


def draw_slot_wave(key, part):
    rounds = SLOT_DEV
    pairs = (rounds + 1) // 2
    keys = jax.random.split(jax.random.fold_in(key, 17), pairs)
    perms = jax.vmap(lambda k: jax.random.permutation(k, N_LAT))(keys)
    round_ids = jnp.arange(rounds, dtype=jnp.int32)[:, None]
    places = jnp.arange(N_LAT, dtype=jnp.int32)[None, :]
    chosen = perms[round_ids[:, 0] // 2]
    picks = jnp.where(round_ids % 2 == 0, places, N_LAT - 1 - places)
    owner = jnp.take_along_axis(chosen, jnp.broadcast_to(picks, (rounds, N_LAT)), axis=1)
    wave = round_ids * N_LAT + places
    wave = jnp.where(wave < DEG, wave, DEG)
    slot = owner * SLOT_DEV + round_ids
    table = jnp.zeros((SLOTS,), jnp.int32)
    return table.at[slot.reshape(-1)].set(jnp.broadcast_to(wave, (rounds, N_LAT)).reshape(-1).astype(jnp.int32))


def levels(rng, dims, cuts, smallest, high):
    level, own = 1.0, jax.random.fold_in(rng, 6)
    for dim, shards_of in cuts:
        heights = jnp.exp(jax.random.uniform(jax.random.fold_in(own, dim), (shards_of,), jnp.float32, smallest / len(cuts), high / len(cuts)))
        level = level * jnp.repeat(heights, dims[dim] // shards_of).reshape([-1 if axis == dim else 1 for axis in range(len(dims))])
    return level


def noise(key, shape, scale, reach, cuts=(), kind=jnp.bfloat16):
    result = jax.random.normal(key, shape, jnp.float32) * scale
    if len(cuts) > 0:
        result = levels(key, shape, cuts, -0.22, 0.18) * result
    return jnp.clip(result, min=-reach, max=reach).astype(kind)


def setup_inputs(seed: int = 0, part: int = 0) -> dict:
    key_of = jax.random.split(jax.random.key(seed), 6)
    part_keys = jax.random.split(jax.random.fold_in(key_of[5], part), 6)
    field = draw_field(jax.random.fold_in(jax.random.fold_in(key_of[5], part), 71), part)
    gain = jnp.clip(1.0 + 0.18 * jax.random.normal(key_of[1], (C,), jnp.float32), 0.1, 1.9)
    slot_wave = draw_slot_wave(jax.random.fold_in(key_of[5], 71), part)
    legendre = noise(key_of[3], (SLOTS, DEG, NLAT), NLAT ** -0.5, 0.625, ((0, 16),))
    mixing = noise(key_of[4], (SLOTS, 2, C, C), (2 * C) ** -0.5, 0.25, ((0, 16),))
    return {"field": field, "gain": gain, "slot_wave": slot_wave, "legendre": legendre, "mixing": mixing}


def phase_tables(waves, width):
    points = jnp.arange(width, dtype=jnp.int32)
    phase = (waves[:, None] * points[None, :] % width).astype(jnp.float32) * (2.0 * math.pi / width)
    return (jnp.cos(phase), jnp.sin(phase))

def block_weight(mixing):
    real_part = mixing[:, 0]
    imag_part = mixing[:, 1]
    upper = jnp.concatenate([real_part, imag_part], axis=2)
    lower = jnp.concatenate([-imag_part, real_part], axis=2)
    return jnp.concatenate([upper, lower], axis=1)

def reference(field, gain, slot_wave, legendre, mixing):
    values = field.astype(jnp.float32)
    mean = lax.optimization_barrier(jnp.mean(values, axis=(0, 1)))
    var = lax.optimization_barrier(jnp.mean((values - mean) ** 2, axis=(0, 1)))
    normed = ((values - mean) * (gain / jnp.sqrt(var + 1e-05))).astype(jnp.bfloat16)
    cosine, sine = phase_tables(slot_wave, NLON)
    forward = jnp.stack([cosine, -sine]).astype(jnp.bfloat16)
    weight_m = jnp.where(slot_wave == 0, 1.0, 2.0).astype(jnp.float32)[:, None]
    inverse = jnp.stack([weight_m * cosine, -weight_m * sine]).astype(jnp.bfloat16)
    inv_root = 1.0 / math.sqrt(NLON)
    spectrum = jnp.einsum('anc,rkn->karc', normed.astype(jnp.float32), forward.astype(jnp.float32)) * inv_root
    spectrum = spectrum.astype(jnp.bfloat16).reshape(SLOTS, NLAT, 2 * C)
    big = block_weight(mixing)
    lat_scale = math.sqrt(NLAT / DEG)
    degrees = jnp.arange(DEG, dtype=jnp.int32)

    def one_slot(items):
        table, spec, weight, wave = items
        coef = jnp.dot(table, spec, preferred_element_type=jnp.float32)
        coef = jnp.where((degrees >= wave)[:, None], coef, 0.0).astype(jnp.bfloat16)
        mixed = jnp.dot(coef, weight, preferred_element_type=jnp.float32).astype(jnp.bfloat16)
        back = jnp.dot(table.T, mixed, preferred_element_type=jnp.float32) * lat_scale
        return back.astype(jnp.bfloat16)
    back = lax.map(one_slot, (legendre, spectrum, big, slot_wave))
    back = back.reshape(SLOTS, NLAT, 2, C)
    filtered = jnp.einsum('karc,rkn->anc', back.astype(jnp.float32), inverse.astype(jnp.float32)) * inv_root
    return (normed.astype(jnp.float32) + filtered).astype(jnp.bfloat16)
```

```python
import functools
import math

import jax
import jax.numpy as jnp
import numpy as np
from jax import lax
from jax.experimental import pallas as pl
from jax.experimental.pallas import tpu as pltpu
from jax.sharding import PartitionSpec as P

MESH = pl.DeviceIdType.MESH
F32 = jnp.float32
BF16 = jnp.bfloat16


def wave_table(degs, width):
    pad = -(-(degs + 1) // 128) * 128
    waves = np.arange(degs + 1)[:, None]
    phase = (waves * np.arange(width)[None, :] % width) * (2.0 * np.pi / width)
    table = np.zeros((2, pad, width), np.float32)
    table[0, : degs + 1] = np.cos(phase)
    table[1, : degs + 1] = -np.sin(phase)
    return table.reshape(2 * pad, width).astype(BF16), pad


def dot(a, b):
    return jnp.dot(a, b, preferred_element_type=F32)


def partner(me, step, count):
    if count & (count - 1):
        return lax.rem(me + step, count)
    out = 0
    for bit in range(count.bit_length() - 1):
        size = 2**bit
        mine = lax.rem(me // size, 2)
        flip = lax.rem(step // size, 2)
        out = out + size * (mine + flip - 2 * mine * flip)
    return out


def packed_rows(k, count, slot_dev, degs):
    if count % 2 or count * slot_dev != degs:
        return degs + degs
    return 2 * degs + 1 - (4 * k + 2) * count


def exchange_kernel(
    count,
    pad,
    relay,
    kept_rows,
    field_ref, wave_hbm, wave_row_hbm, gain_hbm, table_hbm, tsum_hbm, legendre_hbm, mixing_hbm, back_table_hbm,
    field_v, placed_ref,
    wave_ref, wave_row_ref, gain_ref, table_ref, tsum_row_ref, legendre_ref, mix_v, back_table,
    select, raw, spec, send, recv, back_send, ret, stat_src, stat_recv, lbig, place,
    near_recv, near_back, part_send, part_recv, mixed_send, mixed_recv, pack_send, pack_recv, pack_own, pack_mate,
    field_sem, load_sem, stat_sems, fwd_sems, back_sems, last_sems, pack_sems, part_sems, mixed_sems, near_sems,
):
    me = lax.axis_index("lat")
    lat_dev, width, chans = field_v.shape
    slot_dev, degs, nlat = legendre_ref.shape
    groups, lat_pairs = slot_dev // 2, lat_dev // 2
    rows = count * 8
    others = count - 1
    inv_root = 1.0 / math.sqrt(width)
    total_cells = float(lat_dev * count * width)
    near = count // 2
    side = me // near
    spot = me - side * near
    mate = lax.rem(me + near, count)
    direct = [k for k in range(groups) if k != relay]
    final = direct[-1]
    order = ([relay] if relay is not None else []) + direct
    slot_at = {k: i for i, k in enumerate(direct)}

    barrier = pltpu.get_barrier_semaphore()

    def greet(step, carry):
        pl.semaphore_signal(barrier, inc=1, device_id={"lat": partner(me, step, count)}, device_id_type=MESH)
        return carry

    def load_of(index, source, target):
        load = pltpu.make_async_copy(source, target, load_sem.at[index])
        load.start()
        return load

    row_load = load_of(0, wave_row_hbm, wave_row_ref)
    table_load = load_of(1, table_hbm, table_ref)
    tsum_load = load_of(2, tsum_hbm, tsum_row_ref)
    loads = []
    for a in range(lat_dev):
        load = pltpu.make_async_copy(field_ref.at[a], field_v.at[a], field_sem.at[a])
        load.start()
        loads.append(load)
    late = [
        load_of(3, wave_hbm, wave_ref),
        load_of(4, legendre_hbm, legendre_ref),
        load_of(5, gain_hbm, gain_ref),
        load_of(6, mixing_hbm, mix_v),
        load_of(7, back_table_hbm, back_table),
    ]
    lax.fori_loop(1, count, greet, 0)

    def copy_to(to, source, target, sems):
        pltpu.make_async_remote_copy(
            src_ref=source, dst_ref=target, send_sem=sems.at[0], recv_sem=sems.at[1],
            device_id={"lat": to}, device_id_type=MESH,
        ).start()

    def to_all(source, target, sems):
        def body(step, carry):
            to = partner(me, count - step, count)
            copy_to(to, source(to), target, sems)
            return carry

        lax.fori_loop(1, count, body, 0)

    def to_near(source, target, sems):
        def body(step, carry):
            there = partner(spot, near - step, near)
            copy_to(side * near + there, source(there), target, sems)
            return carry

        lax.fori_loop(1, near, body, 0)

    def wait_bytes(ref, sem):
        pltpu.make_async_copy(ref, ref, sem).wait()

    def merged(block):
        return block.astype(F32).reshape(-1, chans).astype(BF16)

    slots = count * slot_dev
    row_load.wait()
    wave_row = wave_row_ref[...].astype(F32)
    columns = lax.broadcasted_iota(jnp.int32, (rows, 4 * pad), 1).astype(F32)
    row = lax.broadcasted_iota(jnp.int32, (rows, 1), 0)
    slot_lane = lax.broadcasted_iota(jnp.int32, (rows, slots), 1)
    for k in range(groups):
        slot_of = row // 8 * slot_dev + 2 * k + row % 4 // 2
        wave_of = jnp.sum(jnp.where(slot_lane == slot_of, wave_row, 0.0), axis=1, keepdims=True)
        target = wave_of + ((row % 8 // 4 * 2 + row % 2) * pad).astype(F32)
        select[k] = jnp.where(columns == target, 1.0, 0.0).astype(BF16)

    tsum_load.wait()
    part_a = lax.broadcasted_iota(jnp.int32, (2 * pad, 2 * pad), 0)
    part_b = lax.broadcasted_iota(jnp.int32, (2 * pad, 2 * pad), 1)
    tsum_col = jnp.sum(jnp.where(part_a == part_b, tsum_row_ref[...], 0.0), axis=1, keepdims=True)
    table_load.wait()
    sums = jnp.zeros((1, chans), F32)
    for a in range(lat_dev):
        loads[a].wait()
        raw[a] = dot(table_ref[...], field_v[a])
        sums = sums + raw[a, 0:1, :]
    local_mean = sums / float(lat_dev * width)

    half = 2 * pad
    for p in range(lat_pairs):
        for parity in range(2):
            spec[p, parity * half : (parity + 1) * half, :] = (
                raw[2 * p + parity] - tsum_col * local_mean
            ).astype(BF16)

    def pick(k):
        for p in range(lat_pairs):
            picked = dot(select[k], spec[p])
            send[k, :, p] = picked.reshape(count, 8, chans).astype(BF16)

    def start_forward(k):
        i = slot_at[k]
        recv[i, pl.ds(me, 1)] = send[k, pl.ds(me, 1)]
        to_all(lambda to: send.at[k, to], recv.at[i, me], fwd_sems.at[k])

    for load in late:
        load.wait()

    if relay is not None:
        first, second = 2 * relay, 2 * relay + 1
        high = pack_own.shape[0]
        tall, hold = pack_send.shape
        degree_at = lax.broadcasted_iota(jnp.int32, (tall, degs), 1)
        degree_row = lax.broadcasted_iota(jnp.int32, (tall, degs), 0)
        lead = degs - wave_ref[me * slot_dev + first]
        from_first = (degree_row < lead) & (degree_at == degs - 1 - degree_row)
        from_second = (degree_row >= lead) & (degree_row < kept_rows) & (degree_at == degree_row + (degs - kept_rows))
        packed = (
            dot(jnp.where(from_first, 1.0, 0.0).astype(BF16), legendre_ref[first])
            + dot(jnp.where(from_second, 1.0, 0.0).astype(BF16), legendre_ref[second])
        ).astype(BF16)
        lat_in = lax.broadcasted_iota(jnp.int32, (nlat, hold), 0)
        lat_out = lax.broadcasted_iota(jnp.int32, (nlat, hold), 1)
        pack_send[...] = dot(packed, jnp.where(lat_in == lat_out + (1 - side) * hold, 1.0, 0.0).astype(BF16)).astype(BF16)
        packed_near = dot(packed, jnp.where(lat_in == lat_out + side * hold, 1.0, 0.0).astype(BF16)).astype(BF16)
        twice = jnp.where(
            lax.broadcasted_iota(jnp.int32, (high, tall), 0) // 2 == lax.broadcasted_iota(jnp.int32, (high, tall), 1),
            1.0, 0.0,
        ).astype(BF16)
        quad = jnp.where(
            lax.broadcasted_iota(jnp.int32, (hold, 4 * hold), 1) // 4 == lax.broadcasted_iota(jnp.int32, (hold, 4 * hold), 0),
            1.0, 0.0,
        ).astype(BF16)
        line_id = lax.broadcasted_iota(jnp.int32, (high, 4 * hold), 0)
        cell_id = lax.broadcasted_iota(jnp.int32, (high, 4 * hold), 1)

        def widen(block, lead):
            full = dot(dot(twice, block).astype(BF16), quad)
            in_second = jnp.where(line_id // 2 < lead, 0, 1)
            match = (cell_id % 2 == line_id % 2) & (cell_id % 4 // 2 == in_second)
            return jnp.where(match, full, 0.0).astype(BF16)

        pack_own[...] = widen(packed_near, lead)
        packed_full = dot(twice, packed).astype(BF16)
        pick(relay)
        near_recv[0, pl.ds(spot, 1)] = send[relay, pl.ds(me, 1)]
        near_recv[1, pl.ds(spot, 1)] = send[relay, pl.ds(mate, 1)]

    pick(direct[0])
    pl.semaphore_wait(barrier, others)

    if relay is not None:
        copy_to(mate, pack_send, pack_recv, pack_sems)
        to_near(lambda there: send.at[relay, side * near + there], near_recv.at[0, spot], fwd_sems.at[relay])
        to_near(lambda there: send.at[relay, (1 - side) * near + there], near_recv.at[1, spot], fwd_sems.at[relay])
    start_forward(direct[0])

    squares = jnp.zeros((8, chans), F32)
    for a in range(lat_dev):
        values = field_v[a].astype(F32)
        squares = squares + jnp.sum((values * values).reshape(width // 8, 8, chans), axis=0)
    square = jnp.sum(squares, axis=0, keepdims=True)
    own = jnp.concatenate([sums, square], axis=0)
    stat_src[...] = own
    stat_recv[pl.ds(me, 1)] = own[None]
    to_all(lambda to: stat_src, stat_recv.at[me], stat_sems)

    for k in direct[1:]:
        pick(k)

    if relay is not None:
        wait_bytes(pack_recv, pack_sems.at[1])
        pack_mate[...] = widen(pack_recv[...], degs - wave_ref[mate * slot_dev + first])
        wait_bytes(near_recv.at[:, pl.ds(0, near - 1)], fwd_sems.at[relay, 1])
        part_send[...] = dot(pack_mate[...], merged(near_recv[1])).reshape(part_send.shape).astype(BF16)
        copy_to(mate, part_send, part_recv, part_sems)

    for k in direct[1:]:
        start_forward(k)

    slot_a = lax.broadcasted_iota(jnp.int32, (slots, slots), 0)
    slot_b = lax.broadcasted_iota(jnp.int32, (slots, slots), 1)
    wave_col = jnp.sum(jnp.where(slot_a == slot_b, wave_row, 0.0), axis=1, keepdims=True)
    lane = lax.broadcasted_iota(jnp.int32, (1, rows), 1)
    slot_line = lax.broadcasted_iota(jnp.int32, (slots, rows), 0)
    place_line = lax.broadcasted_iota(jnp.int32, (4 * pad, rows), 0).astype(F32)

    def place_of(k):
        slot_of = lane // 8 * slot_dev + 2 * k + lane % 4 // 2
        wave_of = jnp.sum(jnp.where(slot_line == slot_of, wave_col, 0.0), axis=0, keepdims=True)
        target = wave_of + ((lane % 8 // 4 * 2 + lane % 2) * pad).astype(F32)
        return jnp.where(place_line == target, 1.0, 0.0).astype(BF16)

    place[...] = place_of(final)

    col = lax.broadcasted_iota(jnp.int32, (nlat, 4 * nlat), 1)
    lat_row = lax.broadcasted_iota(jnp.int32, (nlat, 4 * nlat), 0)
    degree = lax.broadcasted_iota(jnp.int32, (degs, nlat), 0)
    for k in direct:
        for jj in range(2):
            slot = 2 * k + jj
            wave = wave_ref[me * slot_dev + slot]
            kept = jnp.where(degree >= wave, legendre_ref[slot].astype(F32), 0.0).astype(BF16)
            for r in range(2):
                q = 2 * jj + r
                spread = jnp.where(col == 4 * lat_row + q, 1.0, 0.0).astype(BF16)
                lbig[slot_at[k], q * degs : (q + 1) * degs, :] = dot(kept, spread).astype(BF16)

    wait_bytes(stat_recv.at[pl.ds(0, others)], stat_sems.at[1])
    stats = stat_recv[...]
    total = jnp.sum(stats, axis=0)
    mean = total[0:1] / total_cells
    var = total[1:2] / total_cells - mean * mean
    scale = gain_ref[...] / jnp.sqrt(var + 1e-05)
    shift = (stats[:, 0, :] / float(lat_dev * width) - mean).astype(BF16)

    def owner_rows(copies):
        owner = lax.broadcasted_iota(jnp.int32, (copies * nlat, count), 1)
        lat_of = lax.broadcasted_iota(jnp.int32, (copies * nlat, count), 0)
        span = copies * lat_dev
        owned = jnp.where((lat_of >= owner * span) & (lat_of < (owner + 1) * span), 1.0, 0.0)
        return dot(owned.astype(BF16), shift).astype(BF16)

    mode_scale = scale * inv_root
    lanes = lax.broadcasted_iota(jnp.int32, (1, 2 * pad), 1)
    back_scale = math.sqrt(nlat / degs) * inv_root

    def table_sum(wave, r):
        return jnp.sum(jnp.where(lanes == wave + r * pad, tsum_row_ref[...], 0.0), axis=1, keepdims=True)

    def normalize(a):
        field_v[a] = ((field_v[a].astype(F32) - mean) * scale).astype(BF16)

    normalized = [0]

    def normalize_some(number):
        for a in range(normalized[0], min(lat_dev, normalized[0] + number)):
            normalize(a)
        normalized[0] = min(lat_dev, normalized[0] + number)

    if relay is not None:
        partial = dot(pack_own[...], merged(near_recv[0]))
        offset = dot(packed_full, owner_rows(1))
        line = lax.broadcasted_iota(jnp.int32, (high, 1), 0)
        is_first = line // 2 < lead
        is_real = line % 2 == 0
        waves = [wave_ref[me * slot_dev + first], wave_ref[me * slot_dev + second]]
        sums_of = [jnp.where(is_real, table_sum(w, 0), table_sum(w, 1)) for w in waves]
        partial = partial + jnp.where(is_first, sums_of[0], sums_of[1]) * offset
        weight = jnp.where(is_first, jnp.where(waves[0] == 0, 1.0, 2.0), jnp.where(waves[1] == 0, 1.0, 2.0)) * back_scale
        turn_a = lax.broadcasted_iota(jnp.int32, (high, high), 0)
        turn_b = lax.broadcasted_iota(jnp.int32, (high, high), 1)
        turn = jnp.where(
            (turn_a % 2 == 0) & (turn_b == turn_a + 1), -1.0, jnp.where((turn_a % 2 == 1) & (turn_b == turn_a - 1), 1.0, 0.0)
        ).astype(BF16)
        normalize_some(1)
        wait_bytes(part_recv, part_sems.at[1])
        both = ((partial + part_recv[...].astype(F32).reshape(high, chans)) * mode_scale).astype(BF16)
        turned = dot(turn, both).astype(BF16)
        of_slot = [dot(both, mix_v[s, 0]) + dot(turned, mix_v[s, 1]) for s in (first, second)]
        mixed = (jnp.where(is_first, of_slot[0], of_slot[1]) * weight).astype(BF16)
        mixed_send[...] = mixed.astype(F32).reshape(mixed_send.shape).astype(BF16)
        copy_to(mate, mixed_send, mixed_recv, mixed_sems)

        def expand(which, pack, block):
            back = lax.dot_general(pack, block, (((0,), (0,)), ((), ())), preferred_element_type=F32)
            near_back[which] = back.reshape(near, lat_pairs, 8, chans).astype(BF16)
            owner = me if which == 0 else mate
            ret[relay, pl.ds(owner, 1)] = near_back[which, pl.ds(spot, 1)]
            to_near(lambda there: near_back.at[which, there], ret.at[relay, owner], near_sems.at[which])

        expand(0, pack_own[...], mixed)

    shift_lat = owner_rows(4)

    for k in direct:
        i = slot_at[k]
        normalize_some(3)
        wait_bytes(recv.at[i, pl.ds(0, others)], fwd_sems.at[k, 1])
        arrived = merged(recv[i])
        coef = dot(lbig[i], arrived)
        offset = dot(lbig[i], shift_lat)
        mixed = []
        for jj in range(2):
            slot = 2 * k + jj
            wave = wave_ref[me * slot_dev + slot]
            parts = []
            for r in range(2):
                q = slice((2 * jj + r) * degs, (2 * jj + r + 1) * degs)
                parts.append(((coef[q] + table_sum(wave, r) * offset[q]) * mode_scale).astype(BF16))
            both = jnp.concatenate(parts, axis=0)
            by_real = dot(both, mix_v[slot, 0])
            by_imag = dot(both, mix_v[slot, 1])
            weight = jnp.where(wave == 0, 1.0, 2.0) * back_scale
            mixed.append(((by_real[:degs] - by_imag[degs:]) * weight).astype(BF16))
            mixed.append(((by_imag[:degs] + by_real[degs:]) * weight).astype(BF16))
        mixed = jnp.concatenate(mixed, axis=0)
        back = lax.dot_general(lbig[i], mixed, (((0,), (0,)), ((), ())), preferred_element_type=F32)
        back_send[i] = back.reshape(count, lat_pairs, 8, chans).astype(BF16)
        ret[k, pl.ds(me, 1)] = back_send[i, pl.ds(me, 1)]
        if k != final:
            to_all(lambda to: back_send.at[i, to], ret.at[k, me], back_sems.at[k])
        else:
            to_all(lambda to: back_send.at[i, to, 0], ret.at[k, me, 0], last_sems.at[0])

    if relay is not None:
        wait_bytes(mixed_recv, mixed_sems.at[1])
        expand(1, pack_mate[...], mixed_recv[...].astype(F32).reshape(high, chans).astype(BF16))
    for p in range(1, lat_pairs):
        to_all(lambda to: back_send.at[slot_at[final], to, p], ret.at[final, me, p], last_sems.at[p])
    normalize_some(lat_dev)

    wait_bytes(stat_recv.at[pl.ds(0, others)], stat_sems.at[0])
    for k in direct:
        wait_bytes(recv.at[slot_at[k], pl.ds(0, others)], fwd_sems.at[k, 0])
    if relay is not None:
        wait_bytes(near_recv.at[:, pl.ds(0, near - 1)], fwd_sems.at[relay, 0])
        wait_bytes(pack_recv, pack_sems.at[0])
        wait_bytes(part_recv, part_sems.at[0])
        wait_bytes(mixed_recv, mixed_sems.at[0])
        for which in range(2):
            wait_bytes(ret.at[relay, pl.ds(0, near - 1)], near_sems.at[which, 0])
    for k in direct[:-1]:
        wait_bytes(ret.at[k, pl.ds(0, others)], back_sems.at[k, 0])
        wait_bytes(ret.at[k, pl.ds(0, others)], back_sems.at[k, 1])
    if relay is not None:
        for which in range(2):
            wait_bytes(ret.at[relay, pl.ds(0, near - 1)], near_sems.at[which, 1])
    for k in range(groups):
        if k == final:
            continue
        spot_of = place_of(k)
        for p in range(lat_pairs):
            early = dot(spot_of, merged(ret[k, :, p])).reshape(2, half, chans)
            so_far = slice(2 * p, 2 * p + 2)
            raw[so_far] = early if k == 0 else raw[so_far] + early
    for p in range(lat_pairs):
        wait_bytes(ret.at[final, pl.ds(0, others), p], last_sems.at[p, 0])
        wait_bytes(ret.at[final, pl.ds(0, others), p], last_sems.at[p, 1])
        placed = dot(place[...], merged(ret[final, :, p]))
        if groups > 1:
            placed = placed + raw[2 * p : 2 * p + 2].reshape(4 * pad, chans)
        placed = placed.astype(BF16)
        if p < lat_pairs - 1:
            for parity in range(2):
                a = 2 * p + parity
                filtered = dot(back_table[...], placed[parity * half : (parity + 1) * half])
                field_v[a] = (field_v[a].astype(F32) + filtered).astype(BF16)
        else:
            placed_ref[...] = placed


def finish_kernel(part_ref, placed_ref, back_table_ref, out_hbm, tail, sems):
    lat_dev = part_ref.shape[0]
    half = placed_ref.shape[0] // 2
    copies = []
    for a in range(lat_dev - 2):
        copies.append(pltpu.make_async_copy(part_ref.at[a], out_hbm.at[a], sems.at[a]))
        copies[-1].start()
    for parity in range(2):
        a = lat_dev - 2 + parity
        filtered = dot(back_table_ref[...], placed_ref[parity * half : (parity + 1) * half])
        tail[parity] = (part_ref[a].astype(F32) + filtered).astype(BF16)
        copies.append(pltpu.make_async_copy(tail.at[parity], out_hbm.at[a], sems.at[a]))
        copies[-1].start()
    for copy in copies:
        copy.wait()


def per_device(field, gain, slot_wave, legendre, mixing):
    count = lax.axis_size("lat")
    lat_dev, width, chans = field.shape
    slot_dev, degs, nlat = legendre.shape
    groups, lat_pairs = slot_dev // 2, lat_dev // 2
    table, pad = wave_table(degs, width)
    tsum = table.astype(np.float64).sum(axis=1).astype(np.float32)
    back_table = jnp.asarray(table.T.copy())
    rows = count * 8
    near = count // 2
    kept_rows = packed_rows(groups - 1, count, slot_dev, degs)
    relay = groups - 1 if groups > 1 and 0 < kept_rows < nlat else None
    kept_rows = kept_rows if relay is not None else 8
    high = -(-2 * kept_rows // 8) * 8
    tall = -(-kept_rows // 16) * 16
    straight = groups - (relay is not None)
    vmem = pl.BlockSpec(memory_space=pltpu.VMEM)
    hbm = pl.BlockSpec(memory_space=pltpu.HBM)
    dma = pltpu.SemaphoreType.DMA
    half_limit = 30 * 2**20
    chunk = (lat_pairs, 8, chans)
    part, placed = pl.pallas_call(
        functools.partial(exchange_kernel, count, pad, relay, kept_rows),
        out_shape=(
            jax.ShapeDtypeStruct(field.shape, BF16),
            jax.ShapeDtypeStruct((4 * pad, chans), BF16),
        ),
        in_specs=[hbm] * 9,
        out_specs=(vmem, vmem),
        scratch_shapes=[
            pltpu.SMEM(slot_wave.shape, jnp.int32),
            pltpu.VMEM((1,) + slot_wave.shape, jnp.int32),
            pltpu.VMEM((1, chans), F32),
            pltpu.VMEM(table.shape, BF16),
            pltpu.VMEM((1, 2 * pad), F32),
            pltpu.VMEM(legendre.shape, BF16),
            pltpu.VMEM(mixing.shape, BF16),
            pltpu.VMEM(back_table.shape, BF16),
            pltpu.VMEM((groups, rows, 4 * pad), BF16),
            pltpu.VMEM((lat_dev, 2 * pad, chans), F32),
            pltpu.VMEM((lat_pairs, 4 * pad, chans), BF16),
            pltpu.VMEM((groups, count) + chunk, BF16),
            pltpu.VMEM((straight, count) + chunk, BF16),
            pltpu.VMEM((straight, count) + chunk, BF16),
            pltpu.VMEM((groups, count) + chunk, BF16),
            pltpu.VMEM((2, chans), F32),
            pltpu.VMEM((count, 2, chans), F32),
            pltpu.VMEM((straight, 4 * degs, 4 * nlat), BF16),
            pltpu.VMEM((4 * pad, rows), BF16),
            pltpu.VMEM((2, near) + chunk, BF16),
            pltpu.VMEM((2, near) + chunk, BF16),
            pltpu.VMEM((high // 8, 8, chans), BF16),
            pltpu.VMEM((high // 8, 8, chans), BF16),
            pltpu.VMEM((high // 8, 8, chans), BF16),
            pltpu.VMEM((high // 8, 8, chans), BF16),
            pltpu.VMEM((tall, nlat // 2), BF16),
            pltpu.VMEM((tall, nlat // 2), BF16),
            pltpu.VMEM((high, 2 * nlat), BF16),
            pltpu.VMEM((high, 2 * nlat), BF16),
            dma((lat_dev,)),
            dma((8,)),
            dma((2,)),
            dma((groups, 2)),
            dma((groups, 2)),
            dma((lat_pairs, 2)),
            dma((2,)),
            dma((2,)),
            dma((2,)),
            dma((2, 2)),
        ],
        compiler_params=pltpu.CompilerParams(
            collective_id=0, has_side_effects=True, vmem_limit_bytes=half_limit if count <= 16 else 63 * 2**20
        ),
        name="exchange",
    )(*(pltpu.with_memory_space_constraint(x, pltpu.HBM) for x in (
        field, slot_wave, slot_wave.reshape(1, -1), gain.reshape(1, chans), jnp.asarray(table),
        jnp.asarray(tsum.reshape(1, -1)), legendre, mixing, back_table,
    )))
    return pl.pallas_call(
        finish_kernel,
        out_shape=jax.ShapeDtypeStruct(field.shape, BF16),
        in_specs=[vmem, vmem, vmem],
        out_specs=hbm,
        scratch_shapes=[pltpu.VMEM((2, width, chans), BF16), dma((lat_dev,))],
        compiler_params=pltpu.CompilerParams(vmem_limit_bytes=half_limit),
        name="finish",
    )(part, placed, back_table)


def solution(mesh):
    return jax.shard_map(
        per_device,
        mesh=mesh,
        in_specs=(
            P(("member", "lat"), None, None),
            P(),
            P(),
            P("lat", None, None),
            P("lat", None, None, None),
        ),
        out_specs=P(("member", "lat"), None, None),
        check_vma=False,
    )
```

```python
import functools
import math

import jax
import jax.numpy as jnp
import numpy as np
from jax import lax
from jax.experimental import pallas as pl
from jax.experimental.pallas import tpu as pltpu
from jax.sharding import PartitionSpec as P

MESH = pl.DeviceIdType.MESH
F32 = jnp.float32
BF16 = jnp.bfloat16


def wave_table(degs, slots, width):
    kept = degs if slots == degs and degs % 32 == 0 else degs + 1
    pad = degs if kept == degs else -(-kept // 128) * 128
    waves = np.arange(kept)[:, None]
    phase = (waves * np.arange(width)[None, :] % width) * (2.0 * np.pi / width)
    table = np.zeros((2, pad, width), np.float32)
    table[0, :kept] = np.cos(phase)
    table[1, :kept] = -np.sin(phase)
    return table.reshape(2 * pad, width).astype(BF16), pad


def dot(a, b):
    return jnp.dot(a, b, preferred_element_type=F32)


def partner(me, step, count):
    if count & (count - 1):
        return lax.rem(me + step, count)
    out = 0
    for bit in range(count.bit_length() - 1):
        size = 2**bit
        mine = lax.rem(me // size, 2)
        flip = lax.rem(step // size, 2)
        out = out + size * (mine + flip - 2 * mine * flip)
    return out


def packed_rows(k, count, slot_dev, degs):
    if count % 2 or count * slot_dev != degs:
        return degs + degs
    return 2 * degs + 1 - (4 * k + 2) * count


def exchange_kernel(
    count,
    pad,
    relay,
    kept_rows,
    field_ref, wave_hbm, wave_row_hbm, gain_hbm, table_hbm, tsum_hbm, legendre_hbm, mixing_hbm, back_table_hbm,
    field_v, early_ref, block_ref, place,
    wave_ref, wave_row_ref, gain_ref, table_ref, tsum_row_ref, legendre_ref, mix_v, back_table,
    select, raw, spec, send, recv, back_send, ret, stat_src, stat_recv, lbig,
    near_recv, near_back, part_send, part_recv, mixed_send, mixed_recv, pack_send, pack_recv, pack_own, pack_mate,
    field_sem, load_sem, stat_sems, fwd_sems, back_sems, last_sems, pack_sems, part_sems, mixed_sems, near_sems,
):
    me = lax.axis_index("lat")
    lat_dev, width, chans = field_v.shape
    slot_dev, degs, nlat = legendre_ref.shape
    groups, lat_pairs = slot_dev // 2, lat_dev // 2
    rows = count * 8
    others = count - 1
    inv_root = 1.0 / math.sqrt(width)
    total_cells = float(lat_dev * count * width)
    near = count // 2
    side = me // near
    spot = me - side * near
    mate = lax.rem(me + near, count)
    direct = [k for k in range(groups) if k != relay]
    final = direct[-1]
    order = ([relay] if relay is not None else []) + direct
    slot_at = {k: i for i, k in enumerate(direct)}

    flips = [2**bit * (1 - 2 * lax.rem(me // 2**bit, 2)) for bit in range(count.bit_length() - 1)]

    def peer(step):
        if count & (count - 1):
            return lax.rem(me + step, count)
        to = me
        for bit, flip in enumerate(flips):
            to = to + flip if step >> bit & 1 else to
        return to

    def each_peer(act):
        if count > 16:
            lax.fori_loop(1, count, lambda step, carry: (act(partner(me, count - step, count)), carry)[1], 0)
        else:
            for step in range(count - 1, 0, -1):
                act(peer(step))

    def each_near(act):
        if count > 16 or count & (count - 1):
            lax.fori_loop(1, near, lambda step, carry: (act(side * near + partner(spot, near - step, near)), carry)[1], 0)
        else:
            for step in range(near - 1, 0, -1):
                act(peer(step))

    def each_far(act):
        if count > 16 or count & (count - 1):
            lax.fori_loop(0, near, lambda step, carry: (act((1 - side) * near + lax.rem(spot + step, near)), carry)[1], 0)
        else:
            for step in range(count - 1, near - 1, -1):
                act(peer(step))

    inner = side != spot // max(1, near // 2)
    barrier = pltpu.get_barrier_semaphore()

    def greet(to):
        pl.semaphore_signal(barrier, inc=1, device_id={"lat": to}, device_id_type=MESH)

    each_peer(greet)

    def load_of(index, source, target):
        load = pltpu.make_async_copy(source, target, load_sem.at[index])
        load.start()
        return load

    row_load = load_of(0, wave_row_hbm, wave_row_ref)
    table_load = load_of(1, table_hbm, table_ref)
    tsum_load = load_of(2, tsum_hbm, tsum_row_ref)
    loads = []
    for a in range(lat_dev):
        load = pltpu.make_async_copy(field_ref.at[a], field_v.at[a], field_sem.at[a])
        load.start()
        loads.append(load)
    late = [
        load_of(3, wave_hbm, wave_ref),
        load_of(4, legendre_hbm, legendre_ref),
        load_of(5, gain_hbm, gain_ref),
        load_of(6, mixing_hbm, mix_v),
        load_of(7, back_table_hbm, back_table),
    ]

    def copy_to(to, source, target, sems):
        pltpu.make_async_remote_copy(
            src_ref=source, dst_ref=target, send_sem=sems.at[0], recv_sem=sems.at[1],
            device_id={"lat": to}, device_id_type=MESH,
        ).start()

    def to_all(source, target, sems):
        each_peer(lambda to: copy_to(to, source(to), target, sems))

    def to_near(source, target, sems):
        each_near(lambda to: copy_to(to, source(to - side * near), target, sems))

    def wait_bytes(ref, sem):
        pltpu.make_async_copy(ref, ref, sem).wait()

    def merged(block):
        return block.astype(F32).reshape(-1, chans).astype(BF16)

    slots = count * slot_dev
    row_load.wait()
    wave_row = wave_row_ref[...].astype(F32)
    columns = lax.broadcasted_iota(jnp.int32, (rows, 4 * pad), 1).astype(F32)
    row = lax.broadcasted_iota(jnp.int32, (rows, 1), 0)
    slot_lane = lax.broadcasted_iota(jnp.int32, (rows, slots), 1)
    for k in range(groups):
        slot_of = row // 8 * slot_dev + 2 * k + row % 4 // 2
        wave_of = jnp.sum(jnp.where(slot_lane == slot_of, wave_row, 0.0), axis=1, keepdims=True)
        target = wave_of + ((row % 8 // 4 * 2 + row % 2) * pad).astype(F32)
        select[k] = jnp.where(columns == target, 1.0, 0.0).astype(BF16)

    tsum_load.wait()
    part_a = lax.broadcasted_iota(jnp.int32, (2 * pad, 2 * pad), 0)
    part_b = lax.broadcasted_iota(jnp.int32, (2 * pad, 2 * pad), 1)
    tsum_col = jnp.sum(jnp.where(part_a == part_b, tsum_row_ref[...], 0.0), axis=1, keepdims=True)
    table_load.wait()
    half = 2 * pad

    def pick(k, p):
        picked = dot(select[k], spec[p])
        send[k, :, p] = picked.reshape(count, 8, chans).astype(BF16)

    def start_forward(k, pairs):
        i = slot_at[k]
        recv[i, pl.ds(me, 1), pairs] = send[k, pl.ds(me, 1), pairs]
        to_all(lambda to: send.at[k, to, pairs], recv.at[i, me, pairs], fwd_sems.at[k])

    def start_ahead(pairs):
        i = slot_at[final]

        @pl.when(inner)
        def _():
            each_far(lambda to: copy_to(to, send.at[final, to, pairs], recv.at[i, me, pairs], fwd_sems.at[final]))

    def start_rest():
        i = slot_at[final]
        recv[i, pl.ds(me, 1)] = send[final, pl.ds(me, 1)]

        @pl.when(jnp.logical_not(inner))
        def _():
            each_far(lambda to: copy_to(to, send.at[final, to], recv.at[i, me], fwd_sems.at[final]))

        to_near(lambda there: send.at[final, side * near + there], recv.at[i, me], fwd_sems.at[final])

    def start_near(pairs):
        near_recv[0, pl.ds(spot, 1), pairs] = send[relay, pl.ds(me, 1), pairs]
        near_recv[1, pl.ds(spot, 1), pairs] = send[relay, pl.ds(mate, 1), pairs]
        to_near(lambda there: send.at[relay, side * near + there, pairs], near_recv.at[0, spot, pairs], fwd_sems.at[relay])
        to_near(
            lambda there: send.at[relay, (1 - side) * near + there, pairs], near_recv.at[1, spot, pairs], fwd_sems.at[relay]
        )

    sums = jnp.zeros((1, chans), F32)
    squares = jnp.zeros((8, chans), F32)
    for p in range(lat_pairs):
        for a in (2 * p, 2 * p + 1):
            loads[a].wait()
            raw[a] = dot(table_ref[...], field_v[a])
            sums = sums + raw[a, 0:1, :]
            values = field_v[a].astype(F32)
            squares = squares + jnp.sum((values * values).reshape(width // 8, 8, chans), axis=0)
        if p == 0:
            anchor = sums / float(2 * width)
        for parity in range(2):
            spec[p, parity * half : (parity + 1) * half, :] = (raw[2 * p + parity] - tsum_col * anchor).astype(BF16)
        for k in order[:-1] if len(order) > 1 else order:
            pick(k, p)
        if p == 0:
            pl.semaphore_wait(barrier, others)
        if p == lat_pairs - 1:
            own = jnp.concatenate([sums, jnp.sum(squares, axis=0, keepdims=True), anchor], axis=0)
            stat_src[...] = own
            stat_recv[pl.ds(me, 1)] = own[None]
            to_all(lambda to: stat_src, stat_recv.at[me], stat_sems)
        one = pl.ds(p, 1)
        if relay is not None:
            start_near(one)
        if direct[0] != final or len(order) == 1:
            start_forward(direct[0], one)
        for k in direct[1:-1]:
            start_forward(k, one)
        if len(order) > 1:
            pick(order[-1], p)
            if relay is not None:
                start_ahead(one)
            else:
                start_forward(final, one)
        if p == 0:
            for load in late:
                load.wait()
            if relay is not None:
                first, second = 2 * relay, 2 * relay + 1
                high = pack_own.shape[0]
                tall, hold = pack_send.shape
                degree_at = lax.broadcasted_iota(jnp.int32, (tall, degs), 1)
                degree_row = lax.broadcasted_iota(jnp.int32, (tall, degs), 0)
                lead = degs - wave_ref[me * slot_dev + first]
                from_first = (degree_row < lead) & (degree_at == degs - 1 - degree_row)
                from_second = (
                    (degree_row >= lead) & (degree_row < kept_rows) & (degree_at == degree_row + (degs - kept_rows))
                )
                packed = (
                    dot(jnp.where(from_first, 1.0, 0.0).astype(BF16), legendre_ref[first])
                    + dot(jnp.where(from_second, 1.0, 0.0).astype(BF16), legendre_ref[second])
                ).astype(BF16)
                lat_in = lax.broadcasted_iota(jnp.int32, (nlat, hold), 0)
                lat_out = lax.broadcasted_iota(jnp.int32, (nlat, hold), 1)
                far_lats = jnp.where(lat_in == lat_out + (1 - side) * hold, 1.0, 0.0).astype(BF16)
                pack_send[...] = dot(packed, far_lats).astype(BF16)
                copy_to(mate, pack_send, pack_recv, pack_sems)

    if relay is not None:
        near_lats = jnp.where(lat_in == lat_out + side * hold, 1.0, 0.0).astype(BF16)
        packed_near = dot(packed, near_lats).astype(BF16)
        twice = jnp.where(
            lax.broadcasted_iota(jnp.int32, (high, tall), 0) // 2 == lax.broadcasted_iota(jnp.int32, (high, tall), 1),
            1.0, 0.0,
        ).astype(BF16)
        quad = jnp.where(
            lax.broadcasted_iota(jnp.int32, (hold, 4 * hold), 1) // 4 == lax.broadcasted_iota(jnp.int32, (hold, 4 * hold), 0),
            1.0, 0.0,
        ).astype(BF16)
        line_id = lax.broadcasted_iota(jnp.int32, (high, 4 * hold), 0)
        cell_id = lax.broadcasted_iota(jnp.int32, (high, 4 * hold), 1)

        def widen(block, lead):
            full = dot(dot(twice, block).astype(BF16), quad)
            in_second = jnp.where(line_id // 2 < lead, 0, 1)
            match = (cell_id % 2 == line_id % 2) & (cell_id % 4 // 2 == in_second)
            return jnp.where(match, full, 0.0).astype(BF16)

        pack_own[...] = widen(packed_near, lead)
        packed_full = dot(twice, packed).astype(BF16)
        wait_bytes(pack_recv, pack_sems.at[1])
        pack_mate[...] = widen(pack_recv[...], degs - wave_ref[mate * slot_dev + first])
        wait_bytes(near_recv.at[:, pl.ds(0, near - 1)], fwd_sems.at[relay, 1])
        part_send[...] = dot(pack_mate[...], merged(near_recv[1])).reshape(part_send.shape).astype(BF16)
        for i in range(part_send.shape[0]):
            copy_to(mate, part_send.at[i], part_recv.at[i], part_sems)
        start_rest()

    slot_a = lax.broadcasted_iota(jnp.int32, (slots, slots), 0)
    slot_b = lax.broadcasted_iota(jnp.int32, (slots, slots), 1)
    wave_col = jnp.sum(jnp.where(slot_a == slot_b, wave_row, 0.0), axis=1, keepdims=True)
    lane = lax.broadcasted_iota(jnp.int32, (1, rows), 1)
    slot_line = lax.broadcasted_iota(jnp.int32, (slots, rows), 0)
    place_line = lax.broadcasted_iota(jnp.int32, (4 * pad, rows), 0).astype(F32)

    def place_of(k):
        slot_of = lane // 8 * slot_dev + 2 * k + lane % 4 // 2
        wave_of = jnp.sum(jnp.where(slot_line == slot_of, wave_col, 0.0), axis=0, keepdims=True)
        target = wave_of + ((lane % 8 // 4 * 2 + lane % 2) * pad).astype(F32)
        return jnp.where(place_line == target, 1.0, 0.0).astype(BF16)

    place[...] = place_of(final)

    col = lax.broadcasted_iota(jnp.int32, (nlat, 4 * nlat), 1)
    lat_row = lax.broadcasted_iota(jnp.int32, (nlat, 4 * nlat), 0)
    degree = lax.broadcasted_iota(jnp.int32, (degs, nlat), 0)
    for k in direct:
        for jj in range(2):
            slot = 2 * k + jj
            wave = wave_ref[me * slot_dev + slot]
            kept = jnp.where(degree >= wave, legendre_ref[slot].astype(F32), 0.0).astype(BF16)
            for r in range(2):
                q = 2 * jj + r
                spread = jnp.where(col == 4 * lat_row + q, 1.0, 0.0).astype(BF16)
                lbig[slot_at[k], q * degs : (q + 1) * degs, :] = dot(kept, spread).astype(BF16)

    wait_bytes(stat_recv.at[pl.ds(0, others)], stat_sems.at[1])
    stats = stat_recv[...]
    total = jnp.sum(stats, axis=0)
    mean = total[0:1] / total_cells
    var = total[1:2] / total_cells - mean * mean
    scale = gain_ref[...] / jnp.sqrt(var + 1e-05)
    shift = (stats[:, 2, :] - mean).astype(BF16)

    def owner_rows(copies):
        owner = lax.broadcasted_iota(jnp.int32, (copies * nlat, count), 1)
        lat_of = lax.broadcasted_iota(jnp.int32, (copies * nlat, count), 0)
        span = copies * lat_dev
        owned = jnp.where((lat_of >= owner * span) & (lat_of < (owner + 1) * span), 1.0, 0.0)
        return dot(owned.astype(BF16), shift).astype(BF16)

    mode_scale = scale * inv_root
    lanes = lax.broadcasted_iota(jnp.int32, (1, 2 * pad), 1)
    back_scale = math.sqrt(nlat / degs) * inv_root

    def table_sum(wave, r):
        return jnp.sum(jnp.where(lanes == wave + r * pad, tsum_row_ref[...], 0.0), axis=1, keepdims=True)

    def normalize(a):
        field_v[a] = ((field_v[a].astype(F32) - mean) * scale).astype(BF16)

    normalized = [0]

    def normalize_some(number):
        for a in range(normalized[0], min(lat_dev, normalized[0] + number)):
            normalize(a)
        normalized[0] = min(lat_dev, normalized[0] + number)

    def expand(which, pack, block):
        back = lax.dot_general(pack, block, (((0,), (0,)), ((), ())), preferred_element_type=F32)
        near_back[which] = back.reshape(near, lat_pairs, 8, chans).astype(BF16)
        owner = me if which == 0 else mate
        ret[relay, pl.ds(owner, 1)] = near_back[which, pl.ds(spot, 1)]
        to_near(lambda there: near_back.at[which, there], ret.at[relay, owner], near_sems.at[which])

    def relay_step():
        partial = dot(pack_own[...], merged(near_recv[0]))
        offset = dot(packed_full, owner_rows(1))
        line = lax.broadcasted_iota(jnp.int32, (high, 1), 0)
        is_first = line // 2 < lead
        is_real = line % 2 == 0
        waves = [wave_ref[me * slot_dev + first], wave_ref[me * slot_dev + second]]
        sums_of = [jnp.where(is_real, table_sum(w, 0), table_sum(w, 1)) for w in waves]
        partial = partial + jnp.where(is_first, sums_of[0], sums_of[1]) * offset
        weight = jnp.where(is_first, jnp.where(waves[0] == 0, 1.0, 2.0), jnp.where(waves[1] == 0, 1.0, 2.0)) * back_scale
        turn_a = lax.broadcasted_iota(jnp.int32, (high, high), 0)
        turn_b = lax.broadcasted_iota(jnp.int32, (high, high), 1)
        turn = jnp.where(
            (turn_a % 2 == 0) & (turn_b == turn_a + 1), -1.0, jnp.where((turn_a % 2 == 1) & (turn_b == turn_a - 1), 1.0, 0.0)
        ).astype(BF16)
        wait_bytes(part_recv, part_sems.at[1])
        both = ((partial + part_recv[...].astype(F32).reshape(high, chans)) * mode_scale).astype(BF16)
        turned = dot(turn, both).astype(BF16)
        of_slot = [dot(both, mix_v[s, 0]) + dot(turned, mix_v[s, 1]) for s in (first, second)]
        mixed = (jnp.where(is_first, of_slot[0], of_slot[1]) * weight).astype(BF16)
        mixed_send[...] = mixed.astype(F32).reshape(mixed_send.shape).astype(BF16)
        for i in range(mixed_send.shape[0]):
            copy_to(mate, mixed_send.at[i], mixed_recv.at[i], mixed_sems)

        expand(0, pack_own[...], mixed)

    shift_lat = owner_rows(4)

    def direct_step(k):
        i = slot_at[k]
        wait_bytes(recv.at[i, pl.ds(0, others)], fwd_sems.at[k, 1])
        arrived = merged(recv[i])
        coef = dot(lbig[i], arrived)
        offset = dot(lbig[i], shift_lat)
        mixed = []
        for jj in range(2):
            slot = 2 * k + jj
            wave = wave_ref[me * slot_dev + slot]
            parts = []
            for r in range(2):
                q = slice((2 * jj + r) * degs, (2 * jj + r + 1) * degs)
                parts.append(((coef[q] + table_sum(wave, r) * offset[q]) * mode_scale).astype(BF16))
            both = jnp.concatenate(parts, axis=0)
            by_real = dot(both, mix_v[slot, 0])
            by_imag = dot(both, mix_v[slot, 1])
            weight = jnp.where(wave == 0, 1.0, 2.0) * back_scale
            mixed.append(((by_real[:degs] - by_imag[degs:]) * weight).astype(BF16))
            mixed.append(((by_imag[:degs] + by_real[degs:]) * weight).astype(BF16))
        mixed = jnp.concatenate(mixed, axis=0)
        back = lax.dot_general(lbig[i], mixed, (((0,), (0,)), ((), ())), preferred_element_type=F32)
        back_send[i] = back.reshape(count, lat_pairs, 8, chans).astype(BF16)
        ret[k, pl.ds(me, 1)] = back_send[i, pl.ds(me, 1)]
        start_back(k, pl.ds(0, 1), last_sems.at[0] if k == final else back_sems.at[k])

    def start_back(k, pairs, sems):
        to_all(lambda to: back_send.at[slot_at[k], to, pairs], ret.at[k, me, pairs], sems)

    rest = pl.ds(1, lat_pairs - 1)
    for k in direct:
        direct_step(k)
        if relay is not None and k == direct[max(0, len(direct) - 2)]:
            relay_step()
        if k != final:
            start_back(k, rest, back_sems.at[k])
            normalize_some(2)
    normalize_some(lat_dev)
    if relay is not None:
        wait_bytes(mixed_recv, mixed_sems.at[1])
        expand(1, pack_mate[...], mixed_recv[...].astype(F32).reshape(high, chans).astype(BF16))
    for p in range(1, lat_pairs):
        start_back(final, pl.ds(p, 1), last_sems.at[p])

    wait_bytes(stat_recv.at[pl.ds(0, others)], stat_sems.at[0])
    for k in direct:
        wait_bytes(recv.at[slot_at[k], pl.ds(0, others)], fwd_sems.at[k, 0])
    if relay is not None:
        wait_bytes(near_recv.at[:, pl.ds(0, near - 1)], fwd_sems.at[relay, 0])
        wait_bytes(pack_recv, pack_sems.at[0])
        wait_bytes(part_recv, part_sems.at[0])
        wait_bytes(mixed_recv, mixed_sems.at[0])
        for which in range(2):
            wait_bytes(ret.at[relay, pl.ds(0, near - 1)], near_sems.at[which, 0])
    begun = False
    for k in direct[:-1] + ([relay] if relay is not None else []):
        spot_of = place_of(k)
        for which in range(2):
            if k != relay:
                wait_bytes(ret.at[k, pl.ds(0, others)], back_sems.at[k, which])
            else:
                wait_bytes(ret.at[k, pl.ds(0, near - 1)], near_sems.at[which, 1])
        for p in range(lat_pairs):
            early = dot(spot_of, merged(ret[k, :, p])).reshape(2, half, chans)
            so_far = slice(2 * p, 2 * p + 2)
            raw[so_far] = raw[so_far] + early if begun else early
        begun = True
    if not begun:
        raw[...] = jnp.zeros(raw.shape, F32)
    early_ref[...] = raw[lat_dev - 2 : lat_dev].reshape(4 * pad, chans)
    for p in range(lat_pairs):
        wait_bytes(ret.at[final, pl.ds(0, others), p], last_sems.at[p, 0])
        wait_bytes(ret.at[final, pl.ds(0, others), p], last_sems.at[p, 1])
        block = merged(ret[final, :, p])
        if p == lat_pairs - 1:
            block_ref[...] = block
            continue
        placed = (dot(place[...], block) + raw[2 * p : 2 * p + 2].reshape(4 * pad, chans)).astype(BF16)
        for parity in range(2):
            a = 2 * p + parity
            filtered = dot(back_table[...], placed[parity * half : (parity + 1) * half])
            field_v[a] = (field_v[a].astype(F32) + filtered).astype(BF16)


def finish_kernel(part_ref, early_ref, block_ref, place_ref, back_table_ref, out_hbm, tail, sems):
    lat_dev = part_ref.shape[0]
    width = part_ref.shape[1]
    half = place_ref.shape[0] // 2
    pieces = 3 if width % 48 == 0 else 1
    deep = width // pieces
    copies = []
    for a in range(lat_dev - 2):
        copies.append(pltpu.make_async_copy(part_ref.at[a], out_hbm.at[a], sems.at[a]))
        copies[-1].start()
    placed = (dot(place_ref[...], block_ref[...]) + early_ref[...]).astype(BF16)
    for parity in range(2):
        a = lat_dev - 2 + parity
        for piece in range(pieces):
            lines = pl.ds(piece * deep, deep)
            filtered = dot(back_table_ref[lines, :], placed[parity * half : (parity + 1) * half])
            tail[parity, lines] = (part_ref[a, lines].astype(F32) + filtered).astype(BF16)
            copies.append(
                pltpu.make_async_copy(tail.at[parity, lines], out_hbm.at[a, lines], sems.at[lat_dev + parity * pieces + piece])
            )
            copies[-1].start()
    for copy in copies:
        copy.wait()


def per_device(field, gain, slot_wave, legendre, mixing):
    count = lax.axis_size("lat")
    lat_dev, width, chans = field.shape
    slot_dev, degs, nlat = legendre.shape
    groups, lat_pairs = slot_dev // 2, lat_dev // 2
    table, pad = wave_table(degs, count * slot_dev, width)
    tsum = table.astype(np.float64).sum(axis=1).astype(np.float32)
    back_table = jnp.asarray(table.T.copy())
    rows = count * 8
    near = count // 2
    kept_rows = packed_rows(groups - 1, count, slot_dev, degs)
    relay = groups - 1 if groups > 1 and 0 < kept_rows < nlat else None
    kept_rows = kept_rows if relay is not None else 8
    high = -(-2 * kept_rows // 8) * 8
    tall = -(-kept_rows // 16) * 16
    straight = groups - (relay is not None)
    vmem = pl.BlockSpec(memory_space=pltpu.VMEM)
    hbm = pl.BlockSpec(memory_space=pltpu.HBM)
    dma = pltpu.SemaphoreType.DMA
    half_limit = 30 * 2**20
    chunk = (lat_pairs, 8, chans)
    part, early, block, place = pl.pallas_call(
        functools.partial(exchange_kernel, count, pad, relay, kept_rows),
        out_shape=(
            jax.ShapeDtypeStruct(field.shape, BF16),
            jax.ShapeDtypeStruct((4 * pad, chans), F32),
            jax.ShapeDtypeStruct((rows, chans), BF16),
            jax.ShapeDtypeStruct((4 * pad, rows), BF16),
        ),
        in_specs=[hbm] * 9,
        out_specs=(vmem,) * 4,
        scratch_shapes=[
            pltpu.SMEM(slot_wave.shape, jnp.int32),
            pltpu.VMEM((1,) + slot_wave.shape, jnp.int32),
            pltpu.VMEM((1, chans), F32),
            pltpu.VMEM(table.shape, BF16),
            pltpu.VMEM((1, 2 * pad), F32),
            pltpu.VMEM(legendre.shape, BF16),
            pltpu.VMEM(mixing.shape, BF16),
            pltpu.VMEM(back_table.shape, BF16),
            pltpu.VMEM((groups, rows, 4 * pad), BF16),
            pltpu.VMEM((lat_dev, 2 * pad, chans), F32),
            pltpu.VMEM((lat_pairs, 4 * pad, chans), BF16),
            pltpu.VMEM((groups, count) + chunk, BF16),
            pltpu.VMEM((straight, count) + chunk, BF16),
            pltpu.VMEM((straight, count) + chunk, BF16),
            pltpu.VMEM((groups, count) + chunk, BF16),
            pltpu.VMEM((3, chans), F32),
            pltpu.VMEM((count, 3, chans), F32),
            pltpu.VMEM((straight, 4 * degs, 4 * nlat), BF16),
            pltpu.VMEM((2, near) + chunk, BF16),
            pltpu.VMEM((2, near) + chunk, BF16),
            pltpu.VMEM((high // 8, 8, chans), BF16),
            pltpu.VMEM((high // 8, 8, chans), BF16),
            pltpu.VMEM((high // 8, 8, chans), BF16),
            pltpu.VMEM((high // 8, 8, chans), BF16),
            pltpu.VMEM((tall, nlat // 2), BF16),
            pltpu.VMEM((tall, nlat // 2), BF16),
            pltpu.VMEM((high, 2 * nlat), BF16),
            pltpu.VMEM((high, 2 * nlat), BF16),
            dma((lat_dev,)),
            dma((8,)),
            dma((2,)),
            dma((groups, 2)),
            dma((groups, 2)),
            dma((lat_pairs, 2)),
            dma((2,)),
            dma((2,)),
            dma((2,)),
            dma((2, 2)),
        ],
        compiler_params=pltpu.CompilerParams(
            collective_id=0, has_side_effects=True, vmem_limit_bytes=half_limit if count <= 16 else 63 * 2**20
        ),
        name="exchange",
    )(*(pltpu.with_memory_space_constraint(x, pltpu.HBM) for x in (
        field, slot_wave, slot_wave.reshape(1, -1), gain.reshape(1, chans), jnp.asarray(table),
        jnp.asarray(tsum.reshape(1, -1)), legendre, mixing, back_table,
    )))
    return pl.pallas_call(
        finish_kernel,
        out_shape=jax.ShapeDtypeStruct(field.shape, BF16),
        in_specs=[vmem] * 5,
        out_specs=hbm,
        scratch_shapes=[pltpu.VMEM((2, width, chans), BF16), dma((lat_dev + 6,))],
        compiler_params=pltpu.CompilerParams(vmem_limit_bytes=half_limit),
        name="finish",
    )(part, early, block, place, back_table)


def solution(mesh):
    return jax.shard_map(
        per_device,
        mesh=mesh,
        in_specs=(
            P(("member", "lat"), None, None),
            P(),
            P(),
            P("lat", None, None),
            P("lat", None, None, None),
        ),
        out_specs=P(("member", "lat"), None, None),
        check_vma=False,
    )
```

```python
import functools
import math

import jax
import jax.numpy as jnp
import numpy as np
from jax import lax
from jax.experimental import pallas as pl
from jax.experimental.pallas import tpu as pltpu
from jax.sharding import PartitionSpec as P

MESH = pl.DeviceIdType.MESH
F32 = jnp.float32
BF16 = jnp.bfloat16


def wave_table(degs, slots, width):
    kept = degs if slots == degs and degs % 32 == 0 else degs + 1
    pad = degs if kept == degs else -(-kept // 128) * 128
    waves = np.arange(kept)[:, None]
    phase = (waves * np.arange(width)[None, :] % width) * (2.0 * np.pi / width)
    table = np.zeros((2, pad, width), np.float32)
    table[0, :kept] = np.cos(phase)
    table[1, :kept] = -np.sin(phase)
    return table.reshape(2 * pad, width).astype(BF16), pad


def dot(a, b):
    return jnp.dot(a, b, preferred_element_type=F32)


def partner(me, step, count):
    if count & (count - 1):
        return lax.rem(me + step, count)
    out = 0
    for bit in range(count.bit_length() - 1):
        size = 2**bit
        mine = lax.rem(me // size, 2)
        flip = lax.rem(step // size, 2)
        out = out + size * (mine + flip - 2 * mine * flip)
    return out


def packed_rows(k, count, slot_dev, degs):
    if count % 2 or count * slot_dev != degs:
        return degs + degs
    return 2 * degs + 1 - (4 * k + 2) * count


def exchange_kernel(
    count,
    pad,
    relay,
    kept_rows,
    field_ref, wave_hbm, wave_row_hbm, gain_hbm, table_hbm, tsum_hbm, legendre_hbm, mixing_hbm, back_table_hbm,
    field_v, early_ref, block_ref, place,
    wave_ref, wave_row_ref, gain_ref, table_ref, tsum_row_ref, legendre_ref, mix_v, back_table,
    select, raw, spec, send, recv, back_send, ret, stat_src, stat_recv, sum_send, sum_recv, gap_send, gap_recv, lbig,
    near_recv, near_back, part_send, part_recv, mixed_send, mixed_recv, pack_send, pack_recv, pack_own, pack_mate,
    field_sem, load_sem, stat_sems, fwd_sems, back_sems, last_sems, pack_sems, part_sems, mixed_sems, near_sems,
):
    me = lax.axis_index("lat")
    lat_dev, width, chans = field_v.shape
    slot_dev, degs, nlat = legendre_ref.shape
    groups, lat_pairs = slot_dev // 2, lat_dev // 2
    rows = count * 8
    others = count - 1
    inv_root = 1.0 / math.sqrt(width)
    total_cells = float(lat_dev * count * width)
    near = count // 2
    side = me // near
    spot = me - side * near
    mate = lax.rem(me + near, count)
    direct = [k for k in range(groups) if k != relay]
    final = direct[-1]
    order = ([relay] if relay is not None else []) + direct
    slot_at = {k: i for i, k in enumerate(direct)}
    tails = block_ref.shape[0]

    flips = [2**bit * (1 - 2 * lax.rem(me // 2**bit, 2)) for bit in range(count.bit_length() - 1)]

    def peer(step):
        if count & (count - 1):
            return lax.rem(me + step, count)
        to = me
        for bit, flip in enumerate(flips):
            to = to + flip if step >> bit & 1 else to
        return to

    def each_peer(act):
        if count > 16:
            lax.fori_loop(1, count, lambda step, carry: (act(partner(me, count - step, count)), carry)[1], 0)
        else:
            for step in range(count - 1, 0, -1):
                act(peer(step))

    def each_near(act):
        if count > 16 or count & (count - 1):
            lax.fori_loop(1, near, lambda step, carry: (act(side * near + partner(spot, near - step, near)), carry)[1], 0)
        else:
            for step in range(near - 1, 0, -1):
                act(peer(step))

    def each_far(act):
        if count > 16 or count & (count - 1):
            lax.fori_loop(0, near, lambda step, carry: (act((1 - side) * near + lax.rem(spot + step, near)), carry)[1], 0)
        else:
            for step in range(count - 1, near - 1, -1):
                act(peer(step))

    inner = side != spot // max(1, near // 2)
    barrier = pltpu.get_barrier_semaphore()

    def greet(to):
        pl.semaphore_signal(barrier, inc=1, device_id={"lat": to}, device_id_type=MESH)

    each_peer(greet)

    def load_of(index, source, target):
        load = pltpu.make_async_copy(source, target, load_sem.at[index])
        load.start()
        return load

    row_load = load_of(0, wave_row_hbm, wave_row_ref)
    table_load = load_of(1, table_hbm, table_ref)
    tsum_load = load_of(2, tsum_hbm, tsum_row_ref)
    loads = []
    for a in range(lat_dev):
        load = pltpu.make_async_copy(field_ref.at[a], field_v.at[a], field_sem.at[a])
        load.start()
        loads.append(load)
    late = [
        load_of(3, wave_hbm, wave_ref),
        load_of(4, legendre_hbm, legendre_ref),
        load_of(5, gain_hbm, gain_ref),
        load_of(6, mixing_hbm, mix_v),
        load_of(7, back_table_hbm, back_table),
    ]

    def copy_to(to, source, target, sems):
        pltpu.make_async_remote_copy(
            src_ref=source, dst_ref=target, send_sem=sems.at[0], recv_sem=sems.at[1],
            device_id={"lat": to}, device_id_type=MESH,
        ).start()

    def to_all(source, target, sems):
        each_peer(lambda to: copy_to(to, source(to), target, sems))

    def to_near(source, target, sems):
        each_near(lambda to: copy_to(to, source(to - side * near), target, sems))

    def wait_bytes(ref, sem):
        pltpu.make_async_copy(ref, ref, sem).wait()

    def merged(block):
        return block.astype(F32).reshape(-1, chans).astype(BF16)

    slots = count * slot_dev
    row_load.wait()
    wave_row = wave_row_ref[...].astype(F32)
    columns = lax.broadcasted_iota(jnp.int32, (rows, 4 * pad), 1).astype(F32)
    row = lax.broadcasted_iota(jnp.int32, (rows, 1), 0)
    slot_lane = lax.broadcasted_iota(jnp.int32, (rows, slots), 1)
    for k in range(groups):
        slot_of = row // 8 * slot_dev + 2 * k + row % 4 // 2
        wave_of = jnp.sum(jnp.where(slot_lane == slot_of, wave_row, 0.0), axis=1, keepdims=True)
        target = wave_of + ((row % 8 // 4 * 2 + row % 2) * pad).astype(F32)
        select[k] = jnp.where(columns == target, 1.0, 0.0).astype(BF16)

    tsum_load.wait()
    part_a = lax.broadcasted_iota(jnp.int32, (2 * pad, 2 * pad), 0)
    part_b = lax.broadcasted_iota(jnp.int32, (2 * pad, 2 * pad), 1)
    tsum_col = jnp.sum(jnp.where(part_a == part_b, tsum_row_ref[...], 0.0), axis=1, keepdims=True)
    table_load.wait()
    half = 2 * pad

    def pick(k, p):
        picked = dot(select[k], spec[p])
        send[k, :, p] = picked.reshape(count, 8, chans).astype(BF16)

    def start_forward(k, pairs):
        i = slot_at[k]
        recv[i, pl.ds(me, 1), pairs] = send[k, pl.ds(me, 1), pairs]
        to_all(lambda to: send.at[k, to, pairs], recv.at[i, me, pairs], fwd_sems.at[k])

    def start_ahead(pairs):
        i = slot_at[final]

        @pl.when(inner)
        def _():
            each_far(lambda to: copy_to(to, send.at[final, to, pairs], recv.at[i, me, pairs], fwd_sems.at[final]))

    def start_rest():
        i = slot_at[final]
        recv[i, pl.ds(me, 1)] = send[final, pl.ds(me, 1)]

        @pl.when(jnp.logical_not(inner))
        def _():
            pairs = pl.ds(1, lat_pairs - 1)
            each_far(lambda to: copy_to(to, send.at[final, to, pairs], recv.at[i, me, pairs], fwd_sems.at[final]))

        to_near(lambda there: send.at[final, side * near + there], recv.at[i, me], fwd_sems.at[final])

    def start_near(pairs):
        near_recv[0, pl.ds(spot, 1), pairs] = send[relay, pl.ds(me, 1), pairs]
        near_recv[1, pl.ds(spot, 1), pairs] = send[relay, pl.ds(mate, 1), pairs]
        to_near(lambda there: send.at[relay, side * near + there, pairs], near_recv.at[0, spot, pairs], fwd_sems.at[relay])
        to_near(
            lambda there: send.at[relay, (1 - side) * near + there, pairs], near_recv.at[1, spot, pairs], fwd_sems.at[relay]
        )

    sums = jnp.zeros((1, chans), F32)
    squares = jnp.zeros((8, chans), F32)
    for p in range(lat_pairs):
        loads[2 * p].wait()
        loads[2 * p + 1].wait()
        two = dot(table_ref[...], jnp.concatenate([field_v[2 * p], field_v[2 * p + 1]], axis=1))
        raw[2 * p] = two[:, :chans]
        raw[2 * p + 1] = two[:, chans:]
        for a in (2 * p, 2 * p + 1):
            sums = sums + raw[a, 0:1, :]
            values = field_v[a].astype(F32)
            squares = squares + jnp.sum((values * values).reshape(width // 8, 8, chans), axis=0)
        if p == 0:
            anchor = sums / float(2 * width)
        for parity in range(2):
            spec[p, parity * half : (parity + 1) * half, :] = (raw[2 * p + parity] - tsum_col * anchor).astype(BF16)
        for k in order[:-1] if len(order) > 1 else order:
            pick(k, p)
        if p == 0:
            pl.semaphore_wait(barrier, others)
        if p == lat_pairs - 1:
            own = jnp.concatenate([sums, jnp.sum(squares, axis=0, keepdims=True), anchor], axis=0)
            stat_src[...] = own
            stat_recv[pl.ds(spot, 1)] = own[None]
            to_near(lambda there: stat_src, stat_recv.at[spot], stat_sems.at[0])
        one = pl.ds(p, 1)
        if relay is not None:
            start_near(one)
        if direct[0] != final or len(order) == 1:
            start_forward(direct[0], one)
        for k in direct[1:-1]:
            start_forward(k, one)
        if len(order) > 1:
            pick(order[-1], p)
            if relay is not None:
                start_ahead(one)
            else:
                start_forward(final, one)
        if p == 0:
            for load in late:
                load.wait()
            if relay is not None:
                first, second = 2 * relay, 2 * relay + 1
                high = pack_own.shape[0]
                tall, hold = pack_send.shape
                degree_at = lax.broadcasted_iota(jnp.int32, (tall, degs), 1)
                degree_row = lax.broadcasted_iota(jnp.int32, (tall, degs), 0)
                lead = degs - wave_ref[me * slot_dev + first]
                from_first = (degree_row < lead) & (degree_at == degs - 1 - degree_row)
                from_second = (
                    (degree_row >= lead) & (degree_row < kept_rows) & (degree_at == degree_row + (degs - kept_rows))
                )
                packed = (
                    dot(jnp.where(from_first, 1.0, 0.0).astype(BF16), legendre_ref[first])
                    + dot(jnp.where(from_second, 1.0, 0.0).astype(BF16), legendre_ref[second])
                ).astype(BF16)
                lat_in = lax.broadcasted_iota(jnp.int32, (nlat, hold), 0)
                lat_out = lax.broadcasted_iota(jnp.int32, (nlat, hold), 1)
                far_lats = jnp.where(lat_in == lat_out + (1 - side) * hold, 1.0, 0.0).astype(BF16)
                pack_send[...] = dot(packed, far_lats).astype(BF16)
                copy_to(mate, pack_send, pack_recv, pack_sems)

    if relay is not None:

        @pl.when(jnp.logical_not(inner))
        def _():
            pairs = pl.ds(0, 1)
            each_far(lambda to: copy_to(to, send.at[final, to, pairs], recv.at[slot_at[final], me, pairs], fwd_sems.at[final]))

        near_lats = jnp.where(lat_in == lat_out + side * hold, 1.0, 0.0).astype(BF16)
        packed_near = dot(packed, near_lats).astype(BF16)
        twice = jnp.where(
            lax.broadcasted_iota(jnp.int32, (high, tall), 0) // 2 == lax.broadcasted_iota(jnp.int32, (high, tall), 1),
            1.0, 0.0,
        ).astype(BF16)
        quad = jnp.where(
            lax.broadcasted_iota(jnp.int32, (hold, 4 * hold), 1) // 4 == lax.broadcasted_iota(jnp.int32, (hold, 4 * hold), 0),
            1.0, 0.0,
        ).astype(BF16)
        line_id = lax.broadcasted_iota(jnp.int32, (high, 4 * hold), 0)
        cell_id = lax.broadcasted_iota(jnp.int32, (high, 4 * hold), 1)

        def widen(block, lead):
            full = dot(dot(twice, block).astype(BF16), quad)
            in_second = jnp.where(line_id // 2 < lead, 0, 1)
            match = (cell_id % 2 == line_id % 2) & (cell_id % 4 // 2 == in_second)
            return jnp.where(match, full, 0.0).astype(BF16)

        pack_own[...] = widen(packed_near, lead)
        packed_full = dot(twice, packed).astype(BF16)
    slot_a = lax.broadcasted_iota(jnp.int32, (slots, slots), 0)
    slot_b = lax.broadcasted_iota(jnp.int32, (slots, slots), 1)
    wave_col = jnp.sum(jnp.where(slot_a == slot_b, wave_row, 0.0), axis=1, keepdims=True)
    lane = lax.broadcasted_iota(jnp.int32, (1, rows), 1)
    slot_line = lax.broadcasted_iota(jnp.int32, (slots, rows), 0)
    place_line = lax.broadcasted_iota(jnp.int32, (4 * pad, rows), 0).astype(F32)

    def place_of(k):
        slot_of = lane // 8 * slot_dev + 2 * k + lane % 4 // 2
        wave_of = jnp.sum(jnp.where(slot_line == slot_of, wave_col, 0.0), axis=0, keepdims=True)
        target = wave_of + ((lane % 8 // 4 * 2 + lane % 2) * pad).astype(F32)
        return jnp.where(place_line == target, 1.0, 0.0).astype(BF16)

    place[...] = place_of(final)

    col = lax.broadcasted_iota(jnp.int32, (nlat, 4 * nlat), 1)
    lat_row = lax.broadcasted_iota(jnp.int32, (nlat, 4 * nlat), 0)
    degree = lax.broadcasted_iota(jnp.int32, (degs, nlat), 0)
    for k in direct:
        for jj in range(2):
            slot = 2 * k + jj
            wave = wave_ref[me * slot_dev + slot]
            kept = jnp.where(degree >= wave, legendre_ref[slot].astype(F32), 0.0).astype(BF16)
            for r in range(2):
                q = 2 * jj + r
                spread = jnp.where(col == 4 * lat_row + q, 1.0, 0.0).astype(BF16)
                lbig[slot_at[k], q * degs : (q + 1) * degs, :] = dot(kept, spread).astype(BF16)

    wait_bytes(stat_recv.at[pl.ds(0, near - 1)], stat_sems.at[0, 1])
    stats = stat_recv[...]
    near_total = jnp.sum(stats[:, :2, :], axis=0)
    sum_send[...] = near_total
    gap_send[...] = (stats[:, 2, :] - near_total[0:1] / (0.5 * total_cells)).astype(BF16)
    copy_to(mate, sum_send, sum_recv, stat_sems.at[1])
    copy_to(mate, gap_send, gap_recv, stat_sems.at[2])

    if relay is not None:
        wait_bytes(pack_recv, pack_sems.at[1])
        pack_mate[...] = widen(pack_recv[...], degs - wave_ref[mate * slot_dev + first])
        wait_bytes(near_recv.at[:, pl.ds(0, near - 1)], fwd_sems.at[relay, 1])
        part_send[...] = dot(pack_mate[...], merged(near_recv[1])).reshape(part_send.shape).astype(BF16)
        for i in range(part_send.shape[0]):
            copy_to(mate, part_send.at[i], part_recv.at[i], part_sems)
        start_rest()

    wait_bytes(sum_recv, stat_sems.at[1, 1])
    wait_bytes(gap_recv, stat_sems.at[2, 1])
    total = near_total + sum_recv[...]
    mean = total[0:1] / total_cells
    var = total[1:2] / total_cells - mean * mean
    scale = gain_ref[...] / jnp.sqrt(var + 1e-05)
    shift_near = (stats[:, 2, :] - mean).astype(BF16)
    shift_far = (gap_recv[...].astype(F32) + (sum_recv[0:1] / (0.5 * total_cells) - mean)).astype(BF16)

    def owner_rows(copies):
        owner = lax.broadcasted_iota(jnp.int32, (copies * nlat, near), 1)
        lat_of = lax.broadcasted_iota(jnp.int32, (copies * nlat, near), 0)
        span = copies * lat_dev

        def rows_of(first, shift):
            start = (owner + first) * span
            owned = jnp.where((lat_of >= start) & (lat_of < start + span), 1.0, 0.0)
            return dot(owned.astype(BF16), shift)

        return (rows_of(side * near, shift_near) + rows_of((1 - side) * near, shift_far)).astype(BF16)

    mode_scale = scale * inv_root
    lanes = lax.broadcasted_iota(jnp.int32, (1, 2 * pad), 1)
    back_scale = math.sqrt(nlat / degs) * inv_root

    def table_sum(wave, r):
        return jnp.sum(jnp.where(lanes == wave + r * pad, tsum_row_ref[...], 0.0), axis=1, keepdims=True)

    def normalize(a):
        field_v[a] = ((field_v[a].astype(F32) - mean) * scale).astype(BF16)

    normalized = [0]

    def normalize_some(number):
        for a in range(normalized[0], min(lat_dev, normalized[0] + number)):
            normalize(a)
        normalized[0] = min(lat_dev, normalized[0] + number)

    def expand(which, pack, block):
        back = lax.dot_general(pack, block, (((0,), (0,)), ((), ())), preferred_element_type=F32)
        near_back[which] = back.reshape(near, lat_pairs, 8, chans).astype(BF16)
        owner = me if which == 0 else mate
        ret[relay, pl.ds(owner, 1)] = near_back[which, pl.ds(spot, 1)]
        to_near(lambda there: near_back.at[which, there], ret.at[relay, owner], near_sems.at[which])

    def relay_step():
        partial = dot(pack_own[...], merged(near_recv[0]))
        offset = dot(packed_full, owner_rows(1))
        line = lax.broadcasted_iota(jnp.int32, (high, 1), 0)
        is_first = line // 2 < lead
        is_real = line % 2 == 0
        waves = [wave_ref[me * slot_dev + first], wave_ref[me * slot_dev + second]]
        sums_of = [jnp.where(is_real, table_sum(w, 0), table_sum(w, 1)) for w in waves]
        partial = partial + jnp.where(is_first, sums_of[0], sums_of[1]) * offset
        weight = jnp.where(is_first, jnp.where(waves[0] == 0, 1.0, 2.0), jnp.where(waves[1] == 0, 1.0, 2.0)) * back_scale
        turn_a = lax.broadcasted_iota(jnp.int32, (high, high), 0)
        turn_b = lax.broadcasted_iota(jnp.int32, (high, high), 1)
        turn = jnp.where(
            (turn_a % 2 == 0) & (turn_b == turn_a + 1), -1.0, jnp.where((turn_a % 2 == 1) & (turn_b == turn_a - 1), 1.0, 0.0)
        ).astype(BF16)
        wait_bytes(part_recv, part_sems.at[1])
        both = ((partial + part_recv[...].astype(F32).reshape(high, chans)) * mode_scale).astype(BF16)
        turned = dot(turn, both).astype(BF16)
        of_slot = [dot(both, mix_v[s, 0]) + dot(turned, mix_v[s, 1]) for s in (first, second)]
        mixed = (jnp.where(is_first, of_slot[0], of_slot[1]) * weight).astype(BF16)
        mixed_send[...] = mixed.astype(F32).reshape(mixed_send.shape).astype(BF16)
        for i in range(mixed_send.shape[0]):
            copy_to(mate, mixed_send.at[i], mixed_recv.at[i], mixed_sems)

        expand(0, pack_own[...], mixed)

    shift_lat = owner_rows(4)

    def direct_step(k):
        i = slot_at[k]
        wait_bytes(recv.at[i, pl.ds(0, others)], fwd_sems.at[k, 1])
        arrived = merged(recv[i])
        coef = dot(lbig[i], arrived)
        offset = dot(lbig[i], shift_lat)
        mixed = []
        for jj in range(2):
            slot = 2 * k + jj
            wave = wave_ref[me * slot_dev + slot]
            parts = []
            for r in range(2):
                q = slice((2 * jj + r) * degs, (2 * jj + r + 1) * degs)
                parts.append(((coef[q] + table_sum(wave, r) * offset[q]) * mode_scale).astype(BF16))
            both = jnp.concatenate(parts, axis=0)
            by_real = dot(both, mix_v[slot, 0])
            by_imag = dot(both, mix_v[slot, 1])
            weight = jnp.where(wave == 0, 1.0, 2.0) * back_scale
            mixed.append(((by_real[:degs] - by_imag[degs:]) * weight).astype(BF16))
            mixed.append(((by_imag[:degs] + by_real[degs:]) * weight).astype(BF16))
        mixed = jnp.concatenate(mixed, axis=0)
        back = lax.dot_general(lbig[i], mixed, (((0,), (0,)), ((), ())), preferred_element_type=F32)
        back_send[i] = back.reshape(count, lat_pairs, 8, chans).astype(BF16)
        ret[k, pl.ds(me, 1)] = back_send[i, pl.ds(me, 1)]
        start_back(k, pl.ds(0, 1), last_sems.at[0] if k == final else back_sems.at[k])

    def start_back(k, pairs, sems):
        to_all(lambda to: back_send.at[slot_at[k], to, pairs], ret.at[k, me, pairs], sems)

    rest = pl.ds(1, lat_pairs - 1)
    for k in direct:
        direct_step(k)
        if relay is not None and k == direct[max(0, len(direct) - 2)]:
            relay_step()
        if k != final:
            start_back(k, rest, back_sems.at[k])
            normalize_some(2)
    normalize_some(lat_dev)
    if relay is not None:
        wait_bytes(mixed_recv, mixed_sems.at[1])
        expand(1, pack_mate[...], mixed_recv[...].astype(F32).reshape(high, chans).astype(BF16))
    for p in range(1, lat_pairs):
        start_back(final, pl.ds(p, 1), last_sems.at[p])

    wait_bytes(stat_recv.at[pl.ds(0, near - 1)], stat_sems.at[0, 0])
    wait_bytes(sum_recv, stat_sems.at[1, 0])
    wait_bytes(gap_recv, stat_sems.at[2, 0])
    for k in direct:
        wait_bytes(recv.at[slot_at[k], pl.ds(0, others)], fwd_sems.at[k, 0])
    if relay is not None:
        wait_bytes(near_recv.at[:, pl.ds(0, near - 1)], fwd_sems.at[relay, 0])
        wait_bytes(pack_recv, pack_sems.at[0])
        wait_bytes(part_recv, part_sems.at[0])
        wait_bytes(mixed_recv, mixed_sems.at[0])
        for which in range(2):
            wait_bytes(ret.at[relay, pl.ds(0, near - 1)], near_sems.at[which, 0])
    begun = False
    for k in direct[:-1] + ([relay] if relay is not None else []):
        spot_of = place_of(k)
        for which in range(2):
            if k != relay:
                wait_bytes(ret.at[k, pl.ds(0, others)], back_sems.at[k, which])
            else:
                wait_bytes(ret.at[k, pl.ds(0, near - 1)], near_sems.at[which, 1])
        for p in range(lat_pairs):
            early = dot(spot_of, merged(ret[k, :, p])).reshape(2, half, chans)
            so_far = slice(2 * p, 2 * p + 2)
            raw[so_far] = raw[so_far] + early if begun else early
        begun = True
    if not begun:
        raw[...] = jnp.zeros(raw.shape, F32)
    early_ref[...] = raw[lat_dev - 2 * tails : lat_dev].reshape(tails, 4 * pad, chans)
    for p in range(lat_pairs):
        wait_bytes(ret.at[final, pl.ds(0, others), p], last_sems.at[p, 0])
        wait_bytes(ret.at[final, pl.ds(0, others), p], last_sems.at[p, 1])
        block = merged(ret[final, :, p])
        if p >= lat_pairs - tails:
            block_ref[p - lat_pairs + tails] = block
            continue
        placed = (dot(place[...], block) + raw[2 * p : 2 * p + 2].reshape(4 * pad, chans)).astype(BF16)
        for parity in range(2):
            a = 2 * p + parity
            filtered = dot(back_table[...], placed[parity * half : (parity + 1) * half])
            field_v[a] = (field_v[a].astype(F32) + filtered).astype(BF16)


def finish_kernel(part_ref, early_ref, block_ref, place_ref, back_table_ref, out_hbm, tail, sems):
    lat_dev = part_ref.shape[0]
    width = part_ref.shape[1]
    half = place_ref.shape[0] // 2
    pieces = 3 if width % 48 == 0 else 1
    deep = width // pieces
    copies = []
    tails, chans = block_ref.shape[0], block_ref.shape[2]
    done = lat_dev - 2 * tails
    for a in range(done):
        copies.append(pltpu.make_async_copy(part_ref.at[a], out_hbm.at[a], sems.at[a]))
        copies[-1].start()
    for t in range(tails):
        placed = (dot(place_ref[...], block_ref[t]) + early_ref[t]).astype(BF16)
        for parity in range(2):
            a = done + 2 * t + parity
            for piece in range(pieces):
                lines = pl.ds(piece * deep, deep)
                filtered = dot(back_table_ref[lines, :], placed[parity * half : (parity + 1) * half])
                tail[2 * t + parity, lines] = (part_ref[a, lines].astype(F32) + filtered).astype(BF16)
                copies.append(
                    pltpu.make_async_copy(
                        tail.at[2 * t + parity, lines], out_hbm.at[a, lines], sems.at[lat_dev + (2 * t + parity) * pieces + piece]
                    )
                )
                copies[-1].start()
    for copy in copies:
        copy.wait()


def per_device(field, gain, slot_wave, legendre, mixing):
    count = lax.axis_size("lat")
    lat_dev, width, chans = field.shape
    slot_dev, degs, nlat = legendre.shape
    groups, lat_pairs = slot_dev // 2, lat_dev // 2
    table, pad = wave_table(degs, count * slot_dev, width)
    tsum = table.astype(np.float64).sum(axis=1).astype(np.float32)
    back_table = jnp.asarray(table.T.copy())
    rows = count * 8
    near = count // 2
    kept_rows = packed_rows(groups - 1, count, slot_dev, degs)
    relay = groups - 1 if groups > 1 and 0 < kept_rows < nlat else None
    kept_rows = kept_rows if relay is not None else 8
    high = -(-2 * kept_rows // 8) * 8
    tall = -(-kept_rows // 16) * 16
    straight = groups - (relay is not None)
    tails = min(2, lat_pairs)
    vmem = pl.BlockSpec(memory_space=pltpu.VMEM)
    hbm = pl.BlockSpec(memory_space=pltpu.HBM)
    dma = pltpu.SemaphoreType.DMA
    half_limit = 30 * 2**20
    chunk = (lat_pairs, 8, chans)
    part, early, block, place = pl.pallas_call(
        functools.partial(exchange_kernel, count, pad, relay, kept_rows),
        out_shape=(
            jax.ShapeDtypeStruct(field.shape, BF16),
            jax.ShapeDtypeStruct((tails, 4 * pad, chans), F32),
            jax.ShapeDtypeStruct((tails, rows, chans), BF16),
            jax.ShapeDtypeStruct((4 * pad, rows), BF16),
        ),
        in_specs=[hbm] * 9,
        out_specs=(vmem,) * 4,
        scratch_shapes=[
            pltpu.SMEM(slot_wave.shape, jnp.int32),
            pltpu.VMEM((1,) + slot_wave.shape, jnp.int32),
            pltpu.VMEM((1, chans), F32),
            pltpu.VMEM(table.shape, BF16),
            pltpu.VMEM((1, 2 * pad), F32),
            pltpu.VMEM(legendre.shape, BF16),
            pltpu.VMEM(mixing.shape, BF16),
            pltpu.VMEM(back_table.shape, BF16),
            pltpu.VMEM((groups, rows, 4 * pad), BF16),
            pltpu.VMEM((lat_dev, 2 * pad, chans), F32),
            pltpu.VMEM((lat_pairs, 4 * pad, chans), BF16),
            pltpu.VMEM((groups, count) + chunk, BF16),
            pltpu.VMEM((straight, count) + chunk, BF16),
            pltpu.VMEM((straight, count) + chunk, BF16),
            pltpu.VMEM((groups, count) + chunk, BF16),
            pltpu.VMEM((3, chans), F32),
            pltpu.VMEM((near, 3, chans), F32),
            pltpu.VMEM((2, chans), F32),
            pltpu.VMEM((2, chans), F32),
            pltpu.VMEM((near, chans), BF16),
            pltpu.VMEM((near, chans), BF16),
            pltpu.VMEM((straight, 4 * degs, 4 * nlat), BF16),
            pltpu.VMEM((2, near) + chunk, BF16),
            pltpu.VMEM((2, near) + chunk, BF16),
            pltpu.VMEM((high // 8, 8, chans), BF16),
            pltpu.VMEM((high // 8, 8, chans), BF16),
            pltpu.VMEM((high // 8, 8, chans), BF16),
            pltpu.VMEM((high // 8, 8, chans), BF16),
            pltpu.VMEM((tall, nlat // 2), BF16),
            pltpu.VMEM((tall, nlat // 2), BF16),
            pltpu.VMEM((high, 2 * nlat), BF16),
            pltpu.VMEM((high, 2 * nlat), BF16),
            dma((lat_dev,)),
            dma((8,)),
            dma((3, 2)),
            dma((groups, 2)),
            dma((groups, 2)),
            dma((lat_pairs, 2)),
            dma((2,)),
            dma((2,)),
            dma((2,)),
            dma((2, 2)),
        ],
        compiler_params=pltpu.CompilerParams(
            collective_id=0, has_side_effects=True, vmem_limit_bytes=half_limit if count <= 16 else 63 * 2**20
        ),
        name="exchange",
    )(*(pltpu.with_memory_space_constraint(x, pltpu.HBM) for x in (
        field, slot_wave, slot_wave.reshape(1, -1), gain.reshape(1, chans), jnp.asarray(table),
        jnp.asarray(tsum.reshape(1, -1)), legendre, mixing, back_table,
    )))
    return pl.pallas_call(
        finish_kernel,
        out_shape=jax.ShapeDtypeStruct(field.shape, BF16),
        in_specs=[vmem] * 5,
        out_specs=hbm,
        scratch_shapes=[pltpu.VMEM((2 * tails, width, chans), BF16), dma((lat_dev + 6 * tails,))],
        compiler_params=pltpu.CompilerParams(vmem_limit_bytes=half_limit),
        name="finish",
    )(part, early, block, place, back_table)


def solution(mesh):
    return jax.shard_map(
        per_device,
        mesh=mesh,
        in_specs=(
            P(("member", "lat"), None, None),
            P(),
            P(),
            P("lat", None, None),
            P("lat", None, None, None),
        ),
        out_specs=P(("member", "lat"), None, None),
        check_vma=False,
    )
```

```python
import functools
import math

import jax
import jax.numpy as jnp
import numpy as np
from jax import lax
from jax.experimental import pallas as pl
from jax.experimental.pallas import tpu as pltpu
from jax.sharding import PartitionSpec as P

MESH = pl.DeviceIdType.MESH
F32 = jnp.float32
BF16 = jnp.bfloat16


def wave_table(degs, slots, width):
    kept = degs if slots == degs and degs % 32 == 0 else degs + 1
    pad = degs if kept == degs else -(-kept // 128) * 128
    waves = np.arange(kept)[:, None]
    phase = (waves * np.arange(width)[None, :] % width) * (2.0 * np.pi / width)
    table = np.zeros((2, pad, width), np.float32)
    table[0, :kept] = np.cos(phase)
    table[1, :kept] = -np.sin(phase)
    return table.reshape(2 * pad, width).astype(BF16), pad


def dot(a, b):
    return jnp.dot(a, b, preferred_element_type=F32)


def partner(me, step, count):
    if count & (count - 1):
        return lax.rem(me + step, count)
    out = 0
    for bit in range(count.bit_length() - 1):
        size = 2**bit
        mine = lax.rem(me // size, 2)
        flip = lax.rem(step // size, 2)
        out = out + size * (mine + flip - 2 * mine * flip)
    return out


def packed_rows(k, count, slot_dev, degs):
    if count % 2 or count * slot_dev != degs:
        return degs + degs
    return 2 * degs + 1 - (4 * k + 2) * count


def exchange_kernel(
    count,
    pad,
    relay,
    kept_rows,
    field_ref, wave_hbm, wave_row_hbm, gain_hbm, table_hbm, tsum_hbm, legendre_hbm, mixing_hbm, back_table_hbm,
    field_v, early_ref, block_ref, place,
    wave_ref, wave_row_ref, gain_ref, table_ref, tsum_row_ref, legendre_ref, mix_v, back_table,
    select, raw, spec, send, recv, back_send, ret, stat_src, stat_recv, sum_send, sum_recv, gap_send, gap_recv, lbig,
    near_recv, near_back, part_send, part_recv, mixed_send, mixed_recv, pack_send, pack_recv, pack_own, pack_mate,
    field_sem, load_sem, stat_sems, fwd_sems, back_sems, last_sems, pack_sems, part_sems, mixed_sems, near_sems,
):
    me = lax.axis_index("lat")
    lat_dev, width, chans = field_v.shape
    slot_dev, degs, nlat = legendre_ref.shape
    groups, lat_pairs = slot_dev // 2, lat_dev // 2
    rows = count * 8
    others = count - 1
    inv_root = 1.0 / math.sqrt(width)
    total_cells = float(lat_dev * count * width)
    near = count // 2
    side = me // near
    spot = me - side * near
    mate = lax.rem(me + near, count)
    direct = [k for k in range(groups) if k != relay]
    final = direct[-1]
    order = ([relay] if relay is not None else []) + direct
    slot_at = {k: i for i, k in enumerate(direct)}
    tails = block_ref.shape[0]

    flips = [2**bit * (1 - 2 * lax.rem(me // 2**bit, 2)) for bit in range(count.bit_length() - 1)]

    def peer(step):
        if count & (count - 1):
            return lax.rem(me + step, count)
        to = me
        for bit, flip in enumerate(flips):
            to = to + flip if step >> bit & 1 else to
        return to

    def each_peer(act):
        if count > 16:
            lax.fori_loop(1, count, lambda step, carry: (act(partner(me, count - step, count)), carry)[1], 0)
        else:
            for step in range(count - 1, 0, -1):
                act(peer(step))

    def each_near(act):
        if count > 16 or count & (count - 1):
            lax.fori_loop(1, near, lambda step, carry: (act(side * near + partner(spot, near - step, near)), carry)[1], 0)
        else:
            for step in range(near - 1, 0, -1):
                act(peer(step))

    def each_far(act):
        if count > 16 or count & (count - 1):
            lax.fori_loop(0, near, lambda step, carry: (act((1 - side) * near + lax.rem(spot + step, near)), carry)[1], 0)
        else:
            for step in range(count - 1, near - 1, -1):
                act(peer(step))

    inner = side != spot // max(1, near // 2)
    barrier = pltpu.get_barrier_semaphore()

    def greet(to):
        pl.semaphore_signal(barrier, inc=1, device_id={"lat": to}, device_id_type=MESH)

    each_peer(greet)

    def load_of(index, source, target):
        load = pltpu.make_async_copy(source, target, load_sem.at[index])
        load.start()
        return load

    row_load = load_of(0, wave_row_hbm, wave_row_ref)
    table_load = load_of(1, table_hbm, table_ref)
    tsum_load = load_of(2, tsum_hbm, tsum_row_ref)
    loads = []
    for a in range(lat_dev):
        load = pltpu.make_async_copy(field_ref.at[a], field_v.at[a], field_sem.at[a])
        load.start()
        loads.append(load)
    late = [
        load_of(3, wave_hbm, wave_ref),
        load_of(4, legendre_hbm, legendre_ref),
        load_of(5, gain_hbm, gain_ref),
        load_of(6, mixing_hbm, mix_v),
        load_of(7, back_table_hbm, back_table),
    ]

    def copy_to(to, source, target, sems):
        pltpu.make_async_remote_copy(
            src_ref=source, dst_ref=target, send_sem=sems.at[0], recv_sem=sems.at[1],
            device_id={"lat": to}, device_id_type=MESH,
        ).start()

    def to_all(source, target, sems):
        each_peer(lambda to: copy_to(to, source(to), target, sems))

    def to_near(source, target, sems):
        each_near(lambda to: copy_to(to, source(to - side * near), target, sems))

    def wait_bytes(ref, sem):
        pltpu.make_async_copy(ref, ref, sem).wait()

    def merged(block):
        return block.astype(F32).reshape(-1, chans).astype(BF16)

    slots = count * slot_dev
    row_load.wait()
    wave_row = wave_row_ref[...].astype(F32)
    columns = lax.broadcasted_iota(jnp.int32, (rows, 4 * pad), 1).astype(F32)
    row = lax.broadcasted_iota(jnp.int32, (rows, 1), 0)
    slot_lane = lax.broadcasted_iota(jnp.int32, (rows, slots), 1)
    for k in range(groups):
        slot_of = row // 8 * slot_dev + 2 * k + row % 4 // 2
        wave_of = jnp.sum(jnp.where(slot_lane == slot_of, wave_row, 0.0), axis=1, keepdims=True)
        target = wave_of + ((row % 8 // 4 * 2 + row % 2) * pad).astype(F32)
        select[k] = jnp.where(columns == target, 1.0, 0.0).astype(BF16)

    tsum_load.wait()
    part_a = lax.broadcasted_iota(jnp.int32, (2 * pad, 2 * pad), 0)
    part_b = lax.broadcasted_iota(jnp.int32, (2 * pad, 2 * pad), 1)
    tsum_col = jnp.sum(jnp.where(part_a == part_b, tsum_row_ref[...], 0.0), axis=1, keepdims=True)
    table_load.wait()
    half = 2 * pad

    def pick(k, p):
        picked = dot(select[k], spec[p])
        send[k, :, p] = picked.reshape(count, 8, chans).astype(BF16)

    def start_forward(k, pairs):
        i = slot_at[k]
        recv[i, pl.ds(me, 1), pairs] = send[k, pl.ds(me, 1), pairs]
        to_all(lambda to: send.at[k, to, pairs], recv.at[i, me, pairs], fwd_sems.at[k])

    def start_ahead(pairs):
        i = slot_at[final]

        @pl.when(inner)
        def _():
            each_far(lambda to: copy_to(to, send.at[final, to, pairs], recv.at[i, me, pairs], fwd_sems.at[final]))

    def start_rest():
        i = slot_at[final]
        recv[i, pl.ds(me, 1)] = send[final, pl.ds(me, 1)]

        @pl.when(jnp.logical_not(inner))
        def _():
            pairs = pl.ds(1, lat_pairs - 1)
            each_far(lambda to: copy_to(to, send.at[final, to, pairs], recv.at[i, me, pairs], fwd_sems.at[final]))


    def start_near(pairs):
        near_recv[0, pl.ds(spot, 1), pairs] = send[relay, pl.ds(me, 1), pairs]
        near_recv[1, pl.ds(spot, 1), pairs] = send[relay, pl.ds(mate, 1), pairs]
        to_near(lambda there: send.at[relay, side * near + there, pairs], near_recv.at[0, spot, pairs], fwd_sems.at[relay])
        to_near(
            lambda there: send.at[relay, (1 - side) * near + there, pairs], near_recv.at[1, spot, pairs], fwd_sems.at[relay]
        )

    sums = jnp.zeros((1, chans), F32)
    squares = jnp.zeros((8, chans), F32)
    for p in range(lat_pairs):
        loads[2 * p].wait()
        loads[2 * p + 1].wait()
        two = dot(table_ref[...], jnp.concatenate([field_v[2 * p], field_v[2 * p + 1]], axis=1))
        raw[2 * p] = two[:, :chans]
        raw[2 * p + 1] = two[:, chans:]
        for a in (2 * p, 2 * p + 1):
            sums = sums + raw[a, 0:1, :]
            values = field_v[a].astype(F32)
            squares = squares + jnp.sum((values * values).reshape(width // 8, 8, chans), axis=0)
        if p == 0:
            anchor = sums / float(2 * width)
        for parity in range(2):
            spec[p, parity * half : (parity + 1) * half, :] = (raw[2 * p + parity] - tsum_col * anchor).astype(BF16)
        for k in order[:-1] if len(order) > 1 else order:
            pick(k, p)
        if p == 0:
            pl.semaphore_wait(barrier, others)
        if p == lat_pairs - 1:
            own = jnp.concatenate([sums, jnp.sum(squares, axis=0, keepdims=True), anchor], axis=0)
            stat_src[...] = own
            stat_recv[pl.ds(spot, 1)] = own[None]
            to_near(lambda there: stat_src, stat_recv.at[spot], stat_sems.at[0])
        one = pl.ds(p, 1)
        if relay is not None:
            start_near(one)
        if direct[0] != final or len(order) == 1:
            start_forward(direct[0], one)
        for k in direct[1:-1]:
            start_forward(k, one)
        if len(order) > 1:
            pick(order[-1], p)
            if relay is not None:
                start_ahead(one)
            else:
                start_forward(final, one)
        if p == 0:
            for load in late:
                load.wait()
            if relay is not None:
                first, second = 2 * relay, 2 * relay + 1
                high = pack_own.shape[0]
                tall, hold = pack_send.shape
                degree_at = lax.broadcasted_iota(jnp.int32, (tall, degs), 1)
                degree_row = lax.broadcasted_iota(jnp.int32, (tall, degs), 0)
                lead = degs - wave_ref[me * slot_dev + first]
                from_first = (degree_row < lead) & (degree_at == degs - 1 - degree_row)
                from_second = (
                    (degree_row >= lead) & (degree_row < kept_rows) & (degree_at == degree_row + (degs - kept_rows))
                )
                packed = (
                    dot(jnp.where(from_first, 1.0, 0.0).astype(BF16), legendre_ref[first])
                    + dot(jnp.where(from_second, 1.0, 0.0).astype(BF16), legendre_ref[second])
                ).astype(BF16)
                lat_in = lax.broadcasted_iota(jnp.int32, (nlat, hold), 0)
                lat_out = lax.broadcasted_iota(jnp.int32, (nlat, hold), 1)
                far_lats = jnp.where(lat_in == lat_out + (1 - side) * hold, 1.0, 0.0).astype(BF16)
                pack_send[...] = dot(packed, far_lats).astype(BF16)
                copy_to(mate, pack_send, pack_recv, pack_sems)

    if relay is not None:

        @pl.when(jnp.logical_not(inner))
        def _():
            pairs = pl.ds(0, 1)
            each_far(lambda to: copy_to(to, send.at[final, to, pairs], recv.at[slot_at[final], me, pairs], fwd_sems.at[final]))

        to_near(lambda there: send.at[final, side * near + there], recv.at[slot_at[final], me], fwd_sems.at[final])
        near_lats = jnp.where(lat_in == lat_out + side * hold, 1.0, 0.0).astype(BF16)
        packed_near = dot(packed, near_lats).astype(BF16)
        twice = jnp.where(
            lax.broadcasted_iota(jnp.int32, (high, tall), 0) // 2 == lax.broadcasted_iota(jnp.int32, (high, tall), 1),
            1.0, 0.0,
        ).astype(BF16)
        quad = jnp.where(
            lax.broadcasted_iota(jnp.int32, (hold, 4 * hold), 1) // 4 == lax.broadcasted_iota(jnp.int32, (hold, 4 * hold), 0),
            1.0, 0.0,
        ).astype(BF16)
        line_id = lax.broadcasted_iota(jnp.int32, (high, 4 * hold), 0)
        cell_id = lax.broadcasted_iota(jnp.int32, (high, 4 * hold), 1)

        def widen(block, lead):
            full = dot(dot(twice, block).astype(BF16), quad)
            in_second = jnp.where(line_id // 2 < lead, 0, 1)
            match = (cell_id % 2 == line_id % 2) & (cell_id % 4 // 2 == in_second)
            return jnp.where(match, full, 0.0).astype(BF16)

        pack_own[...] = widen(packed_near, lead)
        packed_full = dot(twice, packed).astype(BF16)
    slot_a = lax.broadcasted_iota(jnp.int32, (slots, slots), 0)
    slot_b = lax.broadcasted_iota(jnp.int32, (slots, slots), 1)
    wave_col = jnp.sum(jnp.where(slot_a == slot_b, wave_row, 0.0), axis=1, keepdims=True)
    lane = lax.broadcasted_iota(jnp.int32, (1, rows), 1)
    slot_line = lax.broadcasted_iota(jnp.int32, (slots, rows), 0)
    place_line = lax.broadcasted_iota(jnp.int32, (4 * pad, rows), 0).astype(F32)

    def place_of(k):
        slot_of = lane // 8 * slot_dev + 2 * k + lane % 4 // 2
        wave_of = jnp.sum(jnp.where(slot_line == slot_of, wave_col, 0.0), axis=0, keepdims=True)
        target = wave_of + ((lane % 8 // 4 * 2 + lane % 2) * pad).astype(F32)
        return jnp.where(place_line == target, 1.0, 0.0).astype(BF16)

    place[...] = place_of(final)

    col = lax.broadcasted_iota(jnp.int32, (nlat, 4 * nlat), 1)
    lat_row = lax.broadcasted_iota(jnp.int32, (nlat, 4 * nlat), 0)
    degree = lax.broadcasted_iota(jnp.int32, (degs, nlat), 0)
    for k in direct:
        for jj in range(2):
            slot = 2 * k + jj
            wave = wave_ref[me * slot_dev + slot]
            kept = jnp.where(degree >= wave, legendre_ref[slot].astype(F32), 0.0).astype(BF16)
            for r in range(2):
                q = 2 * jj + r
                spread = jnp.where(col == 4 * lat_row + q, 1.0, 0.0).astype(BF16)
                lbig[slot_at[k], q * degs : (q + 1) * degs, :] = dot(kept, spread).astype(BF16)

    wait_bytes(stat_recv.at[pl.ds(0, near - 1)], stat_sems.at[0, 1])
    stats = stat_recv[...]
    near_total = jnp.sum(stats[:, :2, :], axis=0)
    sum_send[...] = near_total
    gap_send[...] = (stats[:, 2, :] - near_total[0:1] / (0.5 * total_cells)).astype(BF16)
    copy_to(mate, sum_send, sum_recv, stat_sems.at[1])
    copy_to(mate, gap_send, gap_recv, stat_sems.at[2])

    if relay is not None:
        wait_bytes(pack_recv, pack_sems.at[1])
        pack_mate[...] = widen(pack_recv[...], degs - wave_ref[mate * slot_dev + first])
        wait_bytes(near_recv.at[:, pl.ds(0, near - 1)], fwd_sems.at[relay, 1])
        part_send[...] = dot(pack_mate[...], merged(near_recv[1])).reshape(part_send.shape).astype(BF16)
        for i in range(part_send.shape[0]):
            copy_to(mate, part_send.at[i], part_recv.at[i], part_sems)
        start_rest()

    wait_bytes(sum_recv, stat_sems.at[1, 1])
    wait_bytes(gap_recv, stat_sems.at[2, 1])
    total = near_total + sum_recv[...]
    mean = total[0:1] / total_cells
    var = total[1:2] / total_cells - mean * mean
    scale = gain_ref[...] / jnp.sqrt(var + 1e-05)
    shift_near = (stats[:, 2, :] - mean).astype(BF16)
    shift_far = (gap_recv[...].astype(F32) + (sum_recv[0:1] / (0.5 * total_cells) - mean)).astype(BF16)

    def owner_rows(copies):
        owner = lax.broadcasted_iota(jnp.int32, (copies * nlat, near), 1)
        lat_of = lax.broadcasted_iota(jnp.int32, (copies * nlat, near), 0)
        span = copies * lat_dev

        def rows_of(first, shift):
            start = (owner + first) * span
            owned = jnp.where((lat_of >= start) & (lat_of < start + span), 1.0, 0.0)
            return dot(owned.astype(BF16), shift)

        return (rows_of(side * near, shift_near) + rows_of((1 - side) * near, shift_far)).astype(BF16)

    mode_scale = scale * inv_root
    lanes = lax.broadcasted_iota(jnp.int32, (1, 2 * pad), 1)
    back_scale = math.sqrt(nlat / degs) * inv_root

    def table_sum(wave, r):
        return jnp.sum(jnp.where(lanes == wave + r * pad, tsum_row_ref[...], 0.0), axis=1, keepdims=True)

    def normalize(a):
        field_v[a] = ((field_v[a].astype(F32) - mean) * scale).astype(BF16)

    normalized = [0]

    def normalize_some(number):
        for a in range(normalized[0], min(lat_dev, normalized[0] + number)):
            normalize(a)
        normalized[0] = min(lat_dev, normalized[0] + number)

    def expand(which, pack, block):
        back = lax.dot_general(pack, block, (((0,), (0,)), ((), ())), preferred_element_type=F32)
        near_back[which] = back.reshape(near, lat_pairs, 8, chans).astype(BF16)
        owner = me if which == 0 else mate
        ret[relay, pl.ds(owner, 1)] = near_back[which, pl.ds(spot, 1)]
        to_near(lambda there: near_back.at[which, there], ret.at[relay, owner], near_sems.at[which])

    def relay_step():
        partial = dot(pack_own[...], merged(near_recv[0]))
        offset = dot(packed_full, owner_rows(1))
        line = lax.broadcasted_iota(jnp.int32, (high, 1), 0)
        is_first = line // 2 < lead
        is_real = line % 2 == 0
        waves = [wave_ref[me * slot_dev + first], wave_ref[me * slot_dev + second]]
        sums_of = [jnp.where(is_real, table_sum(w, 0), table_sum(w, 1)) for w in waves]
        partial = partial + jnp.where(is_first, sums_of[0], sums_of[1]) * offset
        weight = jnp.where(is_first, jnp.where(waves[0] == 0, 1.0, 2.0), jnp.where(waves[1] == 0, 1.0, 2.0)) * back_scale
        turn_a = lax.broadcasted_iota(jnp.int32, (high, high), 0)
        turn_b = lax.broadcasted_iota(jnp.int32, (high, high), 1)
        turn = jnp.where(
            (turn_a % 2 == 0) & (turn_b == turn_a + 1), -1.0, jnp.where((turn_a % 2 == 1) & (turn_b == turn_a - 1), 1.0, 0.0)
        ).astype(BF16)
        wait_bytes(part_recv, part_sems.at[1])
        both = ((partial + part_recv[...].astype(F32).reshape(high, chans)) * mode_scale).astype(BF16)
        turned = dot(turn, both).astype(BF16)
        of_slot = [dot(both, mix_v[s, 0]) + dot(turned, mix_v[s, 1]) for s in (first, second)]
        mixed = (jnp.where(is_first, of_slot[0], of_slot[1]) * weight).astype(BF16)
        mixed_send[...] = mixed.astype(F32).reshape(mixed_send.shape).astype(BF16)
        for i in range(mixed_send.shape[0]):
            copy_to(mate, mixed_send.at[i], mixed_recv.at[i], mixed_sems)

        expand(0, pack_own[...], mixed)

    shift_lat = owner_rows(4)

    def direct_step(k):
        i = slot_at[k]
        wait_bytes(recv.at[i, pl.ds(0, others)], fwd_sems.at[k, 1])
        arrived = merged(recv[i])
        coef = dot(lbig[i], arrived)
        offset = dot(lbig[i], shift_lat)
        mixed = []
        for jj in range(2):
            slot = 2 * k + jj
            wave = wave_ref[me * slot_dev + slot]
            parts = []
            for r in range(2):
                q = slice((2 * jj + r) * degs, (2 * jj + r + 1) * degs)
                parts.append(((coef[q] + table_sum(wave, r) * offset[q]) * mode_scale).astype(BF16))
            both = jnp.concatenate(parts, axis=0)
            by_real = dot(both, mix_v[slot, 0])
            by_imag = dot(both, mix_v[slot, 1])
            weight = jnp.where(wave == 0, 1.0, 2.0) * back_scale
            mixed.append(((by_real[:degs] - by_imag[degs:]) * weight).astype(BF16))
            mixed.append(((by_imag[:degs] + by_real[degs:]) * weight).astype(BF16))
        mixed = jnp.concatenate(mixed, axis=0)
        back = lax.dot_general(lbig[i], mixed, (((0,), (0,)), ((), ())), preferred_element_type=F32)
        back_send[i] = back.reshape(count, lat_pairs, 8, chans).astype(BF16)
        ret[k, pl.ds(me, 1)] = back_send[i, pl.ds(me, 1)]
        start_back(k, pl.ds(0, 1), last_sems.at[0] if k == final else back_sems.at[k])

    def start_back(k, pairs, sems):
        to_all(lambda to: back_send.at[slot_at[k], to, pairs], ret.at[k, me, pairs], sems)

    rest = pl.ds(1, lat_pairs - 1)
    for k in direct:
        direct_step(k)
        if relay is not None and k == direct[max(0, len(direct) - 2)]:
            relay_step()
        if k != final:
            start_back(k, rest, back_sems.at[k])
            normalize_some(2)
    normalize_some(lat_dev)
    if relay is not None:
        wait_bytes(mixed_recv, mixed_sems.at[1])
        expand(1, pack_mate[...], mixed_recv[...].astype(F32).reshape(high, chans).astype(BF16))
    for p in range(1, lat_pairs):
        start_back(final, pl.ds(p, 1), last_sems.at[p])

    begun = False
    for k in direct[:-1] + ([relay] if relay is not None else []):
        spot_of = place_of(k)
        for which in range(2):
            if k != relay:
                wait_bytes(ret.at[k, pl.ds(0, others)], back_sems.at[k, which])
            else:
                wait_bytes(ret.at[k, pl.ds(0, near - 1)], near_sems.at[which, 1])
        for p in range(lat_pairs):
            early = dot(spot_of, merged(ret[k, :, p])).reshape(2, half, chans)
            so_far = slice(2 * p, 2 * p + 2)
            raw[so_far] = raw[so_far] + early if begun else early
        begun = True
    if not begun:
        raw[...] = jnp.zeros(raw.shape, F32)
    early_ref[...] = raw[lat_dev - 2 * tails : lat_dev].reshape(tails, 4 * pad, chans)
    for p in range(lat_pairs):
        wait_bytes(ret.at[final, pl.ds(0, others), p], last_sems.at[p, 0])
        wait_bytes(ret.at[final, pl.ds(0, others), p], last_sems.at[p, 1])
        block = merged(ret[final, :, p])
        if p >= lat_pairs - tails:
            block_ref[p - lat_pairs + tails] = block
            continue
        placed = (dot(place[...], block) + raw[2 * p : 2 * p + 2].reshape(4 * pad, chans)).astype(BF16)
        for parity in range(2):
            a = 2 * p + parity
            filtered = dot(back_table[...], placed[parity * half : (parity + 1) * half])
            field_v[a] = (field_v[a].astype(F32) + filtered).astype(BF16)

    wait_bytes(stat_recv.at[pl.ds(0, near - 1)], stat_sems.at[0, 0])
    wait_bytes(sum_recv, stat_sems.at[1, 0])
    wait_bytes(gap_recv, stat_sems.at[2, 0])
    for k in direct:
        wait_bytes(recv.at[slot_at[k], pl.ds(0, others)], fwd_sems.at[k, 0])
    if relay is not None:
        wait_bytes(near_recv.at[:, pl.ds(0, near - 1)], fwd_sems.at[relay, 0])
        wait_bytes(pack_recv, pack_sems.at[0])
        wait_bytes(part_recv, part_sems.at[0])
        wait_bytes(mixed_recv, mixed_sems.at[0])
        for which in range(2):
            wait_bytes(ret.at[relay, pl.ds(0, near - 1)], near_sems.at[which, 0])


def finish_kernel(part_ref, early_ref, block_ref, place_ref, back_table_ref, out_hbm, tail, sems):
    lat_dev = part_ref.shape[0]
    width = part_ref.shape[1]
    half = place_ref.shape[0] // 2
    pieces = 3 if width % 48 == 0 else 1
    deep = width // pieces
    copies = []
    tails, chans = block_ref.shape[0], block_ref.shape[2]
    done = lat_dev - 2 * tails
    for a in range(done):
        copies.append(pltpu.make_async_copy(part_ref.at[a], out_hbm.at[a], sems.at[a]))
        copies[-1].start()
    for t in range(tails):
        placed = (dot(place_ref[...], block_ref[t]) + early_ref[t]).astype(BF16)
        for parity in range(2):
            a = done + 2 * t + parity
            for piece in range(pieces):
                lines = pl.ds(piece * deep, deep)
                filtered = dot(back_table_ref[lines, :], placed[parity * half : (parity + 1) * half])
                tail[2 * t + parity, lines] = (part_ref[a, lines].astype(F32) + filtered).astype(BF16)
                copies.append(
                    pltpu.make_async_copy(
                        tail.at[2 * t + parity, lines], out_hbm.at[a, lines], sems.at[lat_dev + (2 * t + parity) * pieces + piece]
                    )
                )
                copies[-1].start()
    for copy in copies:
        copy.wait()


def per_device(field, gain, slot_wave, legendre, mixing):
    count = lax.axis_size("lat")
    lat_dev, width, chans = field.shape
    slot_dev, degs, nlat = legendre.shape
    groups, lat_pairs = slot_dev // 2, lat_dev // 2
    table, pad = wave_table(degs, count * slot_dev, width)
    tsum = table.astype(np.float64).sum(axis=1).astype(np.float32)
    back_table = jnp.asarray(table.T.copy())
    rows = count * 8
    near = count // 2
    kept_rows = packed_rows(groups - 1, count, slot_dev, degs)
    relay = groups - 1 if groups > 1 and 0 < kept_rows < nlat else None
    kept_rows = kept_rows if relay is not None else 8
    high = -(-2 * kept_rows // 8) * 8
    tall = -(-kept_rows // 8) * 8
    straight = groups - (relay is not None)
    tails = min(2, lat_pairs)
    vmem = pl.BlockSpec(memory_space=pltpu.VMEM)
    hbm = pl.BlockSpec(memory_space=pltpu.HBM)
    dma = pltpu.SemaphoreType.DMA
    half_limit = 30 * 2**20
    chunk = (lat_pairs, 8, chans)
    part, early, block, place = pl.pallas_call(
        functools.partial(exchange_kernel, count, pad, relay, kept_rows),
        out_shape=(
            jax.ShapeDtypeStruct(field.shape, BF16),
            jax.ShapeDtypeStruct((tails, 4 * pad, chans), F32),
            jax.ShapeDtypeStruct((tails, rows, chans), BF16),
            jax.ShapeDtypeStruct((4 * pad, rows), BF16),
        ),
        in_specs=[hbm] * 9,
        out_specs=(vmem,) * 4,
        scratch_shapes=[
            pltpu.SMEM(slot_wave.shape, jnp.int32),
            pltpu.VMEM((1,) + slot_wave.shape, jnp.int32),
            pltpu.VMEM((1, chans), F32),
            pltpu.VMEM(table.shape, BF16),
            pltpu.VMEM((1, 2 * pad), F32),
            pltpu.VMEM(legendre.shape, BF16),
            pltpu.VMEM(mixing.shape, BF16),
            pltpu.VMEM(back_table.shape, BF16),
            pltpu.VMEM((groups, rows, 4 * pad), BF16),
            pltpu.VMEM((lat_dev, 2 * pad, chans), F32),
            pltpu.VMEM((lat_pairs, 4 * pad, chans), BF16),
            pltpu.VMEM((groups, count) + chunk, BF16),
            pltpu.VMEM((straight, count) + chunk, BF16),
            pltpu.VMEM((straight, count) + chunk, BF16),
            pltpu.VMEM((groups, count) + chunk, BF16),
            pltpu.VMEM((3, chans), F32),
            pltpu.VMEM((near, 3, chans), F32),
            pltpu.VMEM((2, chans), F32),
            pltpu.VMEM((2, chans), F32),
            pltpu.VMEM((near, chans), BF16),
            pltpu.VMEM((near, chans), BF16),
            pltpu.VMEM((straight, 4 * degs, 4 * nlat), BF16),
            pltpu.VMEM((2, near) + chunk, BF16),
            pltpu.VMEM((2, near) + chunk, BF16),
            pltpu.VMEM((high // 8, 8, chans), BF16),
            pltpu.VMEM((high // 8, 8, chans), BF16),
            pltpu.VMEM((high // 8, 8, chans), BF16),
            pltpu.VMEM((high // 8, 8, chans), BF16),
            pltpu.VMEM((tall, nlat // 2), BF16),
            pltpu.VMEM((tall, nlat // 2), BF16),
            pltpu.VMEM((high, 2 * nlat), BF16),
            pltpu.VMEM((high, 2 * nlat), BF16),
            dma((lat_dev,)),
            dma((8,)),
            dma((3, 2)),
            dma((groups, 2)),
            dma((groups, 2)),
            dma((lat_pairs, 2)),
            dma((2,)),
            dma((2,)),
            dma((2,)),
            dma((2, 2)),
        ],
        compiler_params=pltpu.CompilerParams(
            collective_id=0, has_side_effects=True, vmem_limit_bytes=half_limit if count <= 16 else 63 * 2**20
        ),
        name="exchange",
    )(*(pltpu.with_memory_space_constraint(x, pltpu.HBM) for x in (
        field, slot_wave, slot_wave.reshape(1, -1), gain.reshape(1, chans), jnp.asarray(table),
        jnp.asarray(tsum.reshape(1, -1)), legendre, mixing, back_table,
    )))
    return pl.pallas_call(
        finish_kernel,
        out_shape=jax.ShapeDtypeStruct(field.shape, BF16),
        in_specs=[vmem] * 5,
        out_specs=hbm,
        scratch_shapes=[pltpu.VMEM((2 * tails, width, chans), BF16), dma((lat_dev + 6 * tails,))],
        compiler_params=pltpu.CompilerParams(vmem_limit_bytes=half_limit),
        name="finish",
    )(part, early, block, place, back_table)


def solution(mesh):
    return jax.shard_map(
        per_device,
        mesh=mesh,
        in_specs=(
            P(("member", "lat"), None, None),
            P(),
            P(),
            P("lat", None, None),
            P("lat", None, None, None),
        ),
        out_specs=P(("member", "lat"), None, None),
        check_vma=False,
    )
```
